512 devices in a mesh: tm: 16 (over y, core), rows: 32 (over z, x).
Axes of the slice: x: 4, y: 8, z: 8, core: 2. Of those that a mesh axis runs over, the one named last changes fastest.
Arguments:
- features: bfloat16 [16, 96, 64, 512], P('tm', 'rows'), may hold values from -64 to 64, as said below
- gamma: float32 [512], replicated, may hold values from 0.1 to 1.9
- beta: float32 [512], replicated, may hold values from -3 to 3
- kernel: bfloat16 [3, 512, 3, 3, 512], P(None, 'tm'), may hold values from -0.0546875 to 0.0546875
- bias: float32 [512], replicated, may hold values from -3 to 3
Outputs:
- decoded: bfloat16 [16, 96, 64, 512], P('tm', 'rows')
The draws below stay inside these ranges and needn't reach their ends.
Inputs may be any that keep to these rules, and one draw needn't show every extreme that they name: features are finite.
All inputs are finite; a program needn't handle non-finite values.
Results may differ from the reference program's by a relative error of at most 0.004.
Values may be sent and summed in bfloat16 or wider, within the bound.
A program may use at most 128 MiB of HBM per device.

```python
import math
import jax
import jax.numpy as jnp
from jax import lax

C = 512
GROUPS = 32
WIDTH = 64
FRAMES = 16
HEIGHT = 96


def draw_features(key, part):
    first = jax.random.fold_in(key, 0)
    second = jax.random.fold_in(key, 1)
    fourth = jax.random.fold_in(key, 3)
    time_pos = jnp.arange(FRAMES, dtype=jnp.float32) / max(FRAMES - 1, 1)
    row_pos = jnp.arange(HEIGHT, dtype=jnp.float32) / max(HEIGHT - 1, 1)
    time_scale = 0.6 * jnp.exp(time_pos * math.log(3.0))
    row_scale = 0.6 * jnp.exp(row_pos * math.log(3.0))
    rising = time_scale[:, None, None, None] * row_scale[None, :, None, None]
    base = jnp.clip(jax.random.normal(first, (FRAMES, HEIGHT, WIDTH, C), jnp.float32), -6.0, 6.0)
    chan = jnp.exp(jax.random.uniform(second, (C,), jnp.float32, math.log(0.5), math.log(2.0)))
    offset = jax.random.uniform(fourth, (C,), jnp.float32, -1.5, 1.5)
    result = (base * chan + offset) * rising
    return result.astype(jnp.bfloat16)


def levels(key, extent, pieces, low, largest):
    loudness, own = 1.0, jax.random.fold_in(key, 6)
    for dim, blocks in pieces:
        heights = jnp.exp(jax.random.uniform(jax.random.fold_in(own, dim), (blocks,), jnp.float32, low / len(pieces), largest / len(pieces)))
        loudness = loudness * jnp.repeat(heights, extent[dim] // blocks).reshape([-1 if axis == dim else 1 for axis in range(len(extent))])
    return loudness


def scatter_about(own_key, dims, scale, bound, cuts=(), held_as=jnp.bfloat16):
    gain = levels(own_key, dims, cuts, -0.22, 0.18) if cuts else 1.0
    drawn = jax.random.normal(own_key, dims, jnp.float32) * scale * gain
    return jnp.minimum(jnp.maximum(drawn, -bound), bound).astype(held_as)


def setup_inputs(seed: int = 0) -> dict:
    splits = jax.random.split(jax.random.key(seed), 6)
    features = draw_features(jax.random.fold_in(splits[5], 71), 0)
    gamma = jnp.clip(1.0 + 0.18 * jax.random.normal(splits[1], (C,), jnp.float32), 0.1, 1.9)
    beta = scatter_about(splits[2], (C,), 0.5, 3.0, (), jnp.float32)
    kernel = scatter_about(splits[3], (3, C, 3, 3, C), (27 * C) ** -0.5, 0.0546875, ((1, 16),))
    bias = scatter_about(splits[4], (C,), 0.5, 3.0, (), jnp.float32)
    return dict(features=features, gamma=gamma, beta=beta, kernel=kernel, bias=bias)


def reference(features, gamma, beta, kernel, bias):
    frames, height, across, channels = features.shape
    values = features.astype(jnp.float32)
    grouped = values.reshape(frames, height, across, GROUPS, channels // GROUPS)
    center = lax.optimization_barrier(jnp.mean(grouped, axis=(0, 1, 2, 4)))
    centered = grouped - center[:, None]
    spread = lax.optimization_barrier(jnp.mean(centered * centered, axis=(0, 1, 2, 4)))
    normed = (centered * lax.rsqrt(spread + 1e-06)[:, None]).reshape(frames, height, across, channels)
    active = jax.nn.silu(normed * gamma + beta).astype(jnp.bfloat16)
    padded = jnp.concatenate([active[0:1], active[0:1], active], axis=0).astype(jnp.float32)
    taps = jnp.transpose(kernel.astype(jnp.float32), (0, 2, 3, 4, 1))
    conv = lax.conv_general_dilated(padded[None], taps, (1, 1, 1), ((0, 0), (1, 1), (1, 1)), dimension_numbers=('NDHWC', 'DHWIO', 'NDHWC'), precision=lax.Precision.HIGHEST, preferred_element_type=jnp.float32)[0]
    return (values + conv + bias).astype(jnp.bfloat16)
```

```python
import functools

import jax
import jax.numpy as jnp
from jax import lax
from jax.experimental import pallas as pl
from jax.experimental.pallas import tpu as pltpu
from jax.sharding import Mesh
from jax.sharding import PartitionSpec as P

GROUPS = 32
EPSILON = 1e-06
TM = ("tm_0", "tm_1")
ROWS = ("rows_0", "rows_1")
HIGHEST = lax.Precision.HIGHEST
MESH = pl.DeviceIdType.MESH
LANES = 128
ORDER = (0, 2, 1)


def conv_kernel(
    sizes, feat, gamma, beta, kern, bias, out,
    frames, taps, unfolded, acc, arrived, ready, result, consts, stat_y, stat_z, stat_x,
    affine, local_sem, tap_send, tap_recv, ring_send, ring_recv, halo_send, halo_recv,
    y_send, y_recv, z_send, z_recv, x_send, x_recv, part_send, part_recv, back_send, back_recv,
):
    ny, nz, nx = sizes
    tms = 2 * ny
    half = ny // 2
    rows, width, channels = feat.shape[1:]
    outs = kern.shape[2] // 3
    group = channels // GROUPS
    wide = (rows + 1) * width
    last = rows - 1

    y, core = lax.axis_index("tm_0"), lax.axis_index("tm_1")
    z, x = lax.axis_index("rows_0"), lax.axis_index("rows_1")
    me = 2 * y + core
    row = z * nx + x
    has_up, has_down = row > 0, row < nz * nx - 1
    up = {
        "rows_0": jnp.where(x > 0, z, lax.rem(z + nz - 1, nz)),
        "rows_1": jnp.where(x > 0, x - 1, nx - 1),
    }
    down = {
        "rows_0": jnp.where(x < nx - 1, z, lax.rem(z + 1, nz)),
        "rows_1": jnp.where(x < nx - 1, x + 1, 0),
    }
    y_next, y_prev = lax.rem(y + 1, ny), lax.rem(y + ny - 1, ny)
    partner = {"tm_1": 1 - core}

    def chip(offset):
        return lax.rem(y + ny + offset, ny)

    def remote(src, dst, send, recv, device):
        return pltpu.make_async_remote_copy(
            src_ref=src, dst_ref=dst, send_sem=send, recv_sem=recv,
            device_id=device, device_id_type=MESH,
        )

    own = pltpu.make_async_copy(feat.at[0], frames.at[y, pl.ds(1, rows)], local_sem.at[0])
    own.start()
    small = [
        pltpu.make_async_copy(ref, consts.at[i], local_sem.at[1 + i])
        for i, ref in enumerate((gamma, beta, bias))
    ]
    for copy in small:
        copy.start()
    block = 3 * outs

    def tap_copy(a, b):
        return pltpu.make_async_copy(
            kern.at[a, b],
            taps.at[pl.ds(pl.multiple_of(core * 3 * block + a * block, 16), block), pl.ds(b * channels, channels)],
            local_sem.at[4 + 3 * a + b],
        )

    for a in range(3):
        for b in range(3):
            tap_copy(a, b).start()

    barrier = pltpu.get_barrier_semaphore()

    def tm_peer(k):
        peer = lax.rem(me + k, tms)
        return {"tm_0": peer // 2, "tm_1": lax.rem(peer, 2)}

    def z_peer(k):
        return {"rows_0": lax.rem(z + k, nz)}

    def x_peer(k):
        return {"rows_1": lax.rem(x + k, nx)}

    def each(count, peer, do):
        if count > 1:

            @pl.loop(1, count)
            def _(k):
                do(peer(k))

    def greet(device):
        pl.semaphore_signal(barrier, inc=1, device_id=device, device_id_type=MESH)

    each(tms, tm_peer, greet)
    each(nz, z_peer, greet)
    each(nx, x_peer, greet)
    crosses_up = jnp.logical_and(has_up, x == 0)
    crosses_down = jnp.logical_and(has_down, x == nx - 1)
    if nx > 1:

        @pl.when(crosses_up)
        def _():
            greet(up)

        @pl.when(crosses_down)
        def _():
            greet(down)

    lane = lax.broadcasted_iota(jnp.int32, (channels, LANES), 1)
    chan = lax.broadcasted_iota(jnp.int32, (channels, LANES), 0)
    member = jnp.where(chan // group == lane, 1.0, 0.0)

    def gather_groups(v):
        return lax.dot_general(v, member, (((1,), (0,)), ((), ())), precision=HIGHEST, preferred_element_type=jnp.float32)

    def spread_groups(v):
        return lax.dot_general(v, member, (((1,), (1,)), ((), ())), precision=HIGHEST, preferred_element_type=jnp.float32)

    own.wait()
    count = rows * width
    values = frames[y, 1 : 1 + rows].reshape(count, channels).astype(jnp.float32)
    mean_c = jnp.sum(values, axis=0, keepdims=True) * (1.0 / count)
    off = values - mean_c
    m2_c = jnp.sum(off * off, axis=0, keepdims=True)
    mean_c8 = jnp.broadcast_to(mean_c, (8, channels))
    mean_g = gather_groups(mean_c8) * (1.0 / group)
    apart = mean_c8 - spread_groups(mean_g)
    m2_g = gather_groups(m2_c + count * (apart * apart))
    stat_y[me] = jnp.concatenate([mean_g[0:1], m2_g[0:1]], axis=0)

    acc[...] = jnp.zeros_like(acc)
    unfolded[rows * width :, :] = jnp.zeros((width, 3 * channels), unfolded.dtype)

    expected = tms - 1 + nz - 1 + nx - 1
    if nx > 1:
        expected = expected + jnp.where(crosses_up, 1, 0) + jnp.where(crosses_down, 1, 0)
    pl.semaphore_wait(barrier, expected)

    def publish(buf, mine, count, peer, send, recv):
        if count > 1:

            @pl.loop(1, count)
            def _(k):
                remote(buf.at[mine], buf.at[mine], send.at[k], recv.at[mine], peer(k)).start()

    def collect(buf, mine, count, send, recv, weight):
        if count > 1:

            @pl.loop(1, count)
            def _(k):
                other = lax.rem(mine + k, count)
                remote(buf.at[other], buf.at[other], send.at[k], recv.at[other], {"tm_0": y_next}).wait_recv()

        means, m2s = buf[:, 0:1, :], buf[:, 1:2, :]
        mean = jnp.sum(means, axis=0) * (1.0 / count)
        gap = means - mean[None]
        m2 = jnp.sum(m2s, axis=0) + weight * jnp.sum(gap * gap, axis=0)
        return jnp.concatenate([mean, m2], axis=0)

    publish(stat_y, me, tms, tm_peer, y_send, y_recv)

    def ring_copy(src, way, chunk):
        at = frames.at[src, 1 + chunk]
        return remote(at, at, ring_send.at[src, way, chunk], ring_recv.at[src, chunk], {"tm_0": y_next if way == 0 else y_prev})

    def halo_copy(src, side):
        at, to = (1, rows + 1) if side == 0 else (rows, 0)
        return remote(
            frames.at[src, at], frames.at[src, to], halo_send.at[src, side], halo_recv.at[src, side], up if side == 0 else down,
        )

    def send_halo(src, chunk):
        if chunk == 0:
            pl.when(has_up)(lambda: halo_copy(src, 0).start())
        if chunk == last:
            pl.when(has_down)(lambda: halo_copy(src, 1).start())

    for chunk in ORDER:
        ring_copy(y, 0, chunk).start()
        ring_copy(y, 1, chunk).start()
    for chunk in (0, last):
        send_halo(y, chunk)

    def tap_remote():
        at = taps.at[pl.ds(pl.multiple_of(core * 3 * block, 16), 3 * block)]
        return remote(at, at, tap_send, tap_recv, partner)

    for a in range(3):
        for b in range(3):
            tap_copy(a, b).wait()
    tap_remote().start()

    def ring_event(step, chunk):
        for way in (0, 1):
            src = chip(-step) if way == 0 else chip(step)

            def arrive(src=src, way=way):
                ring_copy(src, way, chunk).wait_recv()
                if step < half - 1:
                    ring_copy(src, way, chunk).start()
                elif step == half - 1:
                    pl.when(core == way)(lambda: ring_copy(src, way, chunk).start())
                send_halo(src, chunk)

            if step < half:
                arrive()
            else:
                pl.when(core == way)(arrive)

    for copy in small:
        copy.wait()
    per_device = float(rows * width * group)
    for chunk in ORDER:
        if half > 2 and chunk == ORDER[0]:
            pass
    stat_z[z] = collect(stat_y, me, tms, y_send, y_recv, per_device)
    publish(stat_z, z, nz, z_peer, z_send, z_recv)
    pre = [(step, chunk) for step in range(1, half - 1) for chunk in ORDER]
    cut = len(pre) * 2 // 3
    for step, chunk in pre[:cut]:
        ring_event(step, chunk)
    stat_x[x] = collect(stat_z, z, nz, z_send, z_recv, per_device * tms)
    publish(stat_x, x, nx, x_peer, x_send, x_recv)
    for step, chunk in pre[cut:]:
        ring_event(step, chunk)
    final = collect(stat_x, x, nx, x_send, x_recv, per_device * tms * nz)
    total = per_device * tms * nz * nx
    inv = lax.rsqrt(final[1:2] * (1.0 / total) + EPSILON)
    both = spread_groups(jnp.concatenate([final[0:1], inv] + [jnp.zeros((6, LANES), jnp.float32)], axis=0))
    affine[0:1] = both[0:1]
    affine[1:2] = 0.5 * both[1:2] * consts[0]
    affine[2:3] = 0.5 * consts[1]
    tap_remote().wait_recv()

    column = lax.rem(lax.broadcasted_iota(jnp.int32, (outs, wide), 1), width)
    at_left, at_right = column == 0, column == width - 1

    def process(src):
        for r in (1, rows, 0, rows + 1, *range(2, rows)):
            if r == 0:
                pl.when(has_up)(lambda: halo_copy(src, 1).wait_recv())
            if r == rows + 1:
                pl.when(has_down)(lambda: halo_copy(src, 0).wait_recv())
            value = frames[src, r].astype(jnp.float32)
            h = (value - affine[0:1]) * affine[1:2] + affine[2:3]
            active = h + h * jnp.tanh(h)
            if r == 0:
                active = jnp.where(has_up, active, 0.0)
            if r == rows + 1:
                active = jnp.where(has_down, active, 0.0)
            active = active.astype(unfolded.dtype)
            for b in range(3):
                if 0 <= r - b < rows:
                    unfolded[(r - b) * width : (r - b + 1) * width, b * channels : (b + 1) * channels] = active
        product = lax.dot_general(
            taps[...], unfolded[...], (((1,), (1,)), ((), ())), preferred_element_type=jnp.float32
        )
        frame = 2 * src + core

        for owner in (0, 1):
            for a in range(3):
                base = (owner * 3 + a) * block
                one, two, three = (product[base + c * outs : base + (c + 1) * outs] for c in range(3))
                one = jnp.where(at_left, 0.0, pltpu.roll(one, 1, 1))
                three = jnp.where(at_right, 0.0, pltpu.roll(three, wide - 1, 1))
                total = one + two + three
                acc[owner, frame + 2 - a] += total
                if a < 2:

                    @pl.when(frame == 0)
                    def _():
                        acc[owner, 0] += total
                        if a == 0:
                            acc[owner, 1] += total

    def released(j):
        return chip((j + 1) // 2) if j % 2 else chip(1 - j // 2)

    def part_copy(to):
        return remote(acc.at[1 - core, pl.ds(2 * to, 2)], arrived.at[to], part_send.at[to], part_recv.at[to], partner)

    def back_copy(to, which):
        return remote(
            ready.at[to, which], result.at[me], back_send.at[to, which], back_recv.at[me], {"tm_0": to, "tm_1": which}
        )

    def finish(to):
        part_copy(to).wait_recv()
        for which in (0, 1):
            value = (acc[core, 2 * to + which] + arrived[to, which]).astype(ready.dtype)
            mine = jnp.logical_and(to == y, core == which)

            @pl.when(mine)
            def _():
                result[me] = value

            @pl.when(jnp.logical_not(mine))
            def _():
                ready[to, which] = value
                back_copy(to, which).start()

    def released_at(j):
        return jnp.where(lax.rem(j, 2) == 1, chip((j + 1) // 2), chip(1 - j // 2))

    events = {}
    if half > 1:
        for n, chunk in enumerate(ORDER):
            events.setdefault(min(n, ny - 3), []).append((half - 1, chunk))
    for n, chunk in enumerate(ORDER):
        events.setdefault(ny - 3 + n, []).append((half, chunk))

    @pl.loop(0, ny)
    def _(i):
        for when, todo in events.items():

            @pl.when(i == when)
            def _():
                for step, chunk in todo:
                    ring_event(step, chunk)

        src = chip(jnp.where(lax.rem(i, 2) == 1, (i + 1) // 2, -(i // 2)))
        process(src)

        @pl.when(i > 0)
        def _():
            part_copy(released_at(i)).start()

        @pl.when(i > 1)
        def _():
            finish(released_at(i - 1))

    part_copy(released(ny)).start()
    finish(released(ny - 1))
    finish(released(ny))

    @pl.loop(1, tms)
    def _(k):
        other = lax.rem(me + k, tms)
        remote(result.at[other], result.at[other], back_send.at[0, 0], back_recv.at[other], partner).wait_recv()

    conv = result[...].reshape(channels, wide).astype(jnp.float32)
    conv = jnp.transpose(conv, (1, 0))[: rows * width]
    kept = frames[y, 1 : 1 + rows].reshape(rows * width, channels).astype(jnp.float32)
    total = kept + conv + consts[2]
    out[...] = total.astype(out.dtype).reshape(out.shape)

    def drain(buf, mine, count, send, recv):
        if count > 1:

            @pl.loop(1, count)
            def _(k):
                remote(buf.at[mine], buf.at[mine], send.at[k], recv.at[mine], partner).wait_send()

    drain(stat_y, me, tms, y_send, y_recv)
    drain(stat_z, z, nz, z_send, z_recv)
    drain(stat_x, x, nx, x_send, x_recv)
    tap_remote().wait_send()

    @pl.loop(0, rows)
    def _(chunk):
        for way in (0, 1):
            for step in range(half):
                src = chip(-step) if way == 0 else chip(step)

                def sent(src=src, way=way):
                    ring_copy(src, way, chunk).wait_send()

                if step < half - 1:
                    sent()
                else:
                    pl.when(core == way)(sent)

    @pl.loop(0, ny)
    def _(src):
        pl.when(has_up)(lambda: halo_copy(src, 0).wait_send())
        pl.when(has_down)(lambda: halo_copy(src, 1).wait_send())
        part_copy(src).wait_send()
        for which in (0, 1):

            @pl.when(jnp.logical_not(jnp.logical_and(src == y, core == which)))
            def _():
                back_copy(src, which).wait_send()


def local(sizes, features, gamma, beta, kernel, bias):
    ny, nz, nx = sizes
    tms = 2 * ny
    _, rows, width, channels = features.shape
    outs = kernel.shape[1]
    taps = jnp.transpose(kernel, (0, 2, 3, 1, 4)).reshape(3, 3, 3 * outs, channels)
    wide = (rows + 1) * width
    bf16, f32 = jnp.bfloat16, jnp.float32
    dma = pltpu.SemaphoreType.DMA
    any_spec = pl.BlockSpec(memory_space=pl.ANY)
    vector = lambda v: v.reshape(1, channels)
    return pl.pallas_call(
        functools.partial(conv_kernel, sizes),
        out_shape=jax.ShapeDtypeStruct(features.shape, bf16),
        in_specs=[any_spec] * 5,
        out_specs=pl.BlockSpec(memory_space=pltpu.VMEM),
        scratch_shapes=[
            pltpu.VMEM((ny, rows + 2, width, channels), bf16),
            pltpu.VMEM((18 * outs, 3 * channels), bf16),
            pltpu.VMEM((wide, 3 * channels), bf16),
            pltpu.VMEM((2, tms + 2, outs, wide), f32),
            pltpu.VMEM((ny, 2, outs, wide), f32),
            pltpu.VMEM((ny, 2, outs, wide), bf16),
            pltpu.VMEM((tms, outs, wide), bf16),
            pltpu.VMEM((3, 1, channels), f32),
            pltpu.VMEM((tms, 2, LANES), f32),
            pltpu.VMEM((nz, 2, LANES), f32),
            pltpu.VMEM((nx, 2, LANES), f32),
            pltpu.VMEM((8, channels), f32),
            dma((13,)),
            dma, dma,
            dma((ny, 2, rows)), dma((ny, rows)),
            dma((ny, 2)), dma((ny, 2)),
            dma((tms,)), dma((tms,)),
            dma((nz,)), dma((nz,)),
            dma((nx,)), dma((nx,)),
            dma((ny,)), dma((ny,)),
            dma((ny, 2)), dma((tms,)),
        ],
        compiler_params=pltpu.CompilerParams(collective_id=0, has_side_effects=True, vmem_limit_bytes=60 << 20),
        name="fused_block",
    )(features, vector(gamma), vector(beta), taps, vector(bias))


def solution(mesh):
    sizes = (8, 8, 4)
    split = Mesh(mesh.devices.reshape(8, 2, 8, 4), TM + ROWS)
    in_specs = (P(TM, ROWS, None, None), P(), P(), P(None, TM, None, None, None), P())
    out_specs = P(TM, ROWS, None, None)
    return jax.shard_map(
        functools.partial(local, sizes), mesh=split, in_specs=in_specs, out_specs=out_specs, check_vma=False
    )
```

```python
import functools

import jax
import jax.numpy as jnp
from jax import lax
from jax.experimental import pallas as pl
from jax.experimental.pallas import tpu as pltpu
from jax.sharding import Mesh
from jax.sharding import PartitionSpec as P

GROUPS = 32
EPSILON = 1e-06
TM = ("tm_0", "tm_1")
ROWS = ("rows_0", "rows_1")
HIGHEST = lax.Precision.HIGHEST
MESH = pl.DeviceIdType.MESH
LANES = 128
VMEM_LIMIT = 67043328 - 409600
ORDER = (0, 2, 1)


def conv_kernel(
    sizes, feat, gamma, beta, kern, out,
    frames, taps, wide_a, wide_b, acc, arrived, ready, result, consts, stat_y, stat_z, stat_x,
    affine, local_sem, tap_sem, ring_send, ring_recv, halo_send, halo_recv,
    y_sem, z_sem, x_sem, part_send, part_recv, back_sem,
):
    ny, nz, nx = sizes
    tms = 2 * ny
    half = ny // 2
    rows, width, channels = feat.shape[1:]
    outs = kern.shape[2] // 3
    group = channels // GROUPS
    wide = (rows + 1) * width
    last = rows - 1
    slot = rows + 2

    y, core = lax.axis_index("tm_0"), lax.axis_index("tm_1")
    z, x = lax.axis_index("rows_0"), lax.axis_index("rows_1")
    me = 2 * y + core
    row = z * nx + x
    has_up, has_down = row > 0, row < nz * nx - 1
    inner = jnp.logical_and(has_up, has_down)

    def wrap(v, n):
        v = jnp.where(v >= n, v - n, v)
        return jnp.where(v < 0, v + n, v)

    def chip(offset):
        return wrap(y + offset, ny)

    up = {"rows_0": jnp.where(x > 0, z, wrap(z - 1, nz)), "rows_1": jnp.where(x > 0, x - 1, nx - 1)}
    down = {"rows_0": jnp.where(x < nx - 1, z, wrap(z + 1, nz)), "rows_1": jnp.where(x < nx - 1, x + 1, 0)}
    y_next, y_prev = chip(1), chip(-1)
    partner = {"tm_1": 1 - core}
    home = y * slot

    def remote(src, dst, send, recv, device):
        return pltpu.make_async_remote_copy(
            src_ref=src, dst_ref=dst, send_sem=send, recv_sem=recv,
            device_id=device, device_id_type=MESH,
        )

    own = pltpu.make_async_copy(feat.at[0], frames.at[pl.ds(home + 1, rows)], local_sem.at[0])
    own.start()

    barrier = pltpu.get_barrier_semaphore()

    def far_first(n):
        return sorted(range(1, n), key=lambda k: -min(k, n - k))

    y_peers = [{"tm_0": chip(k), "tm_1": c} for k in far_first(ny) for c in (core, 1 - core)] + [partner]
    z_peers = [{"rows_0": wrap(z + k, nz)} for k in far_first(nz)]
    x_peers = [{"rows_1": wrap(x + k, nx)} for k in far_first(nx)]

    def greet(device):
        pl.semaphore_signal(barrier, inc=1, device_id=device, device_id_type=MESH)

    for peer in y_peers + z_peers + x_peers:
        greet(peer)
    crosses_up = jnp.logical_and(has_up, x == 0)
    crosses_down = jnp.logical_and(has_down, x == nx - 1)
    expected = len(y_peers) + len(z_peers) + len(x_peers)
    if nx > 1:
        pl.when(crosses_up)(lambda: greet(up))
        pl.when(crosses_down)(lambda: greet(down))
        expected = expected + jnp.where(crosses_up, 1, 0) + jnp.where(crosses_down, 1, 0)

    for i, ref in enumerate((gamma, beta)):
        pltpu.make_async_copy(ref, consts.at[i], local_sem.at[1]).start()
    block = 3 * outs
    mine = pl.ds(pl.multiple_of(core * 3 * block, 16), 3 * block)
    for a in range(3):
        for b in range(3):
            pltpu.make_async_copy(
                kern.at[a, b],
                taps.at[pl.ds(pl.multiple_of(core * 3 * block + a * block, 16), block), pl.ds(b * channels, channels)],
                local_sem.at[2],
            ).start()

    lane = lax.broadcasted_iota(jnp.int32, (channels, LANES), 1)
    chan = lax.broadcasted_iota(jnp.int32, (channels, LANES), 0)
    member = jnp.where(chan // group == lane, 1.0, 0.0)

    def gather_groups(v):
        return lax.dot_general(v, member, (((1,), (0,)), ((), ())), precision=HIGHEST, preferred_element_type=jnp.float32)

    def spread_groups(v):
        return lax.dot_general(v, member, (((1,), (1,)), ((), ())), precision=HIGHEST, preferred_element_type=jnp.float32)

    acc[...] = jnp.zeros_like(acc)
    for unfolded in (wide_a, wide_b):
        unfolded[rows * width :, :] = jnp.zeros((width, 3 * channels), unfolded.dtype)

    own.wait()
    count = rows * width
    values = frames[pl.ds(home + 1, rows)].reshape(count, channels).astype(jnp.float32)
    mean_c = jnp.sum(values, axis=0, keepdims=True) * (1.0 / count)
    off = values - mean_c
    m2_c = jnp.sum(off * off, axis=0, keepdims=True)
    mean_c8 = jnp.broadcast_to(mean_c, (8, channels))
    mean_g = gather_groups(mean_c8) * (1.0 / group)
    apart = mean_c8 - spread_groups(mean_g)
    m2_g = gather_groups(m2_c + count * (apart * apart))
    stat_y[me] = jnp.concatenate([mean_g[0:1], m2_g[0:1]], axis=0)

    pl.semaphore_wait(barrier, expected)

    def publish(buf, at, peers, sem):
        for peer in peers:
            remote(buf.at[at], buf.at[at], sem.at[0], sem.at[1], peer).start()

    def several(buf, n, sem):
        return remote(buf.at[pl.ds(0, n)], buf.at[pl.ds(0, n)], sem.at[0], sem.at[1], partner)

    def collect(buf, peers, sem, weight):
        if peers:
            several(buf, len(peers), sem).wait_recv()
        means, m2s = buf[:, 0:1, :], buf[:, 1:2, :]
        mean = jnp.sum(means, axis=0) * (1.0 / buf.shape[0])
        gap = means - mean[None]
        m2 = jnp.sum(m2s, axis=0) + weight * jnp.sum(gap * gap, axis=0)
        return jnp.concatenate([mean, m2], axis=0)

    publish(stat_y, me, y_peers, y_sem)

    def ring_copy(src, way, chunk):
        at = frames.at[src * slot + 1 + chunk]
        return remote(at, at, ring_send, ring_recv.at[src, chunk], {"tm_0": y_next if way == 0 else y_prev})

    def halo_copy(src, side):
        at, to = (1, rows + 1) if side == 0 else (rows, 0)
        return remote(
            frames.at[src * slot + at], frames.at[src * slot + to], halo_send, halo_recv.at[src], up if side == 0 else down
        )

    def send_halo(src, chunk):
        if chunk == 0:
            pl.when(has_up)(lambda: halo_copy(src, 0).start())
        if chunk == last:
            pl.when(has_down)(lambda: halo_copy(src, 1).start())

    for chunk in ORDER:
        ring_copy(y, 0, chunk).start()
        ring_copy(y, 1, chunk).start()
    for chunk in (0, last):
        send_halo(y, chunk)

    pltpu.make_async_copy(taps.at[mine], taps.at[mine], local_sem.at[2]).wait()
    tap_remote = remote(taps.at[mine], taps.at[mine], tap_sem.at[0], tap_sem.at[1], partner)
    tap_remote.start()
    pltpu.make_async_copy(consts, consts, local_sem.at[1]).wait()

    def ring_event(step, chunk):
        for way in (0, 1):
            src = chip(-step) if way == 0 else chip(step)

            def arrive(src=src, way=way):
                ring_copy(src, way, chunk).wait_recv()
                if step < half - 1:
                    ring_copy(src, way, chunk).start()
                elif step == half - 1:
                    pl.when(core == way)(lambda: ring_copy(src, way, chunk).start())
                send_halo(src, chunk)

            if step < half:
                arrive()
            else:
                pl.when(core == way)(arrive)

    per_device = float(rows * width * group)
    early = [(step, chunk) for step in range(1, half - 1) for chunk in ORDER]

    def ring_events(todo):
        for step, chunk in todo:
            ring_event(step, chunk)

    ring_events(early[:1])
    stat_z[z] = collect(stat_y, y_peers, y_sem, per_device)
    publish(stat_z, z, z_peers, z_sem)
    ring_events(early[1:4])
    stat_x[x] = collect(stat_z, z_peers, z_sem, per_device * tms)
    publish(stat_x, x, x_peers, x_sem)
    ring_events(early[4:])
    final = collect(stat_x, x_peers, x_sem, per_device * tms * nz)
    total = per_device * tms * nz * nx
    inv = lax.rsqrt(final[1:2] * (1.0 / total) + EPSILON)
    both = spread_groups(jnp.concatenate([final[0:1], inv] + [jnp.zeros((6, LANES), jnp.float32)], axis=0))
    affine[0:1] = both[0:1]
    affine[1:2] = 0.5 * both[1:2] * consts[0]
    affine[2:3] = 0.5 * consts[1]
    tap_remote.wait_recv()

    column = lax.rem(lax.broadcasted_iota(jnp.int32, (outs, wide), 1), width)
    at_left, at_right = column == 0, column == width - 1

    def source(k):
        if isinstance(k, int):
            return chip((k + 1) // 2 if k % 2 else -(k // 2))
        return chip(jnp.where(lax.rem(k, 2) == 1, (k + 1) // 2, -(k // 2)))

    def halo_wait(src):
        def rows_in(n):
            at = frames.at[pl.ds(0, n)]
            remote(at, at, halo_send, halo_recv.at[src], partner).wait_recv()

        pl.when(inner)(lambda: rows_in(2))
        pl.when(jnp.logical_not(inner))(lambda: rows_in(1))

    def prepare(src, unfolded):
        for r in range(rows + 2):
            value = frames[src * slot + r].astype(jnp.float32)
            h = (value - affine[0:1]) * affine[1:2] + affine[2:3]
            active = h + h * jnp.tanh(h)
            if r == 0:
                active = jnp.where(has_up, active, 0.0)
            if r == rows + 1:
                active = jnp.where(has_down, active, 0.0)
            active = active.astype(unfolded.dtype)
            for b in range(3):
                if 0 <= r - b < rows:
                    unfolded[(r - b) * width : (r - b + 1) * width, b * channels : (b + 1) * channels] = active

    def multiply(src, unfolded):
        frame = 2 * src + core
        totals = []
        for owner in (0, 1):
            product = lax.dot_general(
                taps[owner * 3 * block : (owner + 1) * 3 * block], unfolded[...], (((1,), (1,)), ((), ())),
                preferred_element_type=jnp.float32,
            )
            for a in range(3):
                base = a * block
                one, two, three = (product[base + c * outs : base + (c + 1) * outs] for c in range(3))
                one = jnp.where(at_left, 0.0, pltpu.roll(one, 1, 1))
                three = jnp.where(at_right, 0.0, pltpu.roll(three, wide - 1, 1))
                total = one + two + three
                acc[owner, frame + 2 - a] += total
                totals.append(total)
        return totals

    def repeat_first(src, totals):
        @pl.when(2 * src + core == 0)
        def _():
            for owner in (0, 1):
                acc[owner, 0] += totals[3 * owner] + totals[3 * owner + 1]
                acc[owner, 1] += totals[3 * owner]

    def released(j):
        if isinstance(j, int):
            return chip((j + 1) // 2 if j % 2 else 1 - j // 2)
        return chip(jnp.where(lax.rem(j, 2) == 1, (j + 1) // 2, 1 - j // 2))

    def part_copy(to):
        return remote(acc.at[1 - core, pl.ds(2 * to, 2)], arrived.at[to], part_send, part_recv.at[to], partner)

    low = lax.broadcasted_iota(jnp.int32, (outs // 2, LANES), 1) < width

    def finish(to):
        part_copy(to).wait_recv()
        for which in (0, 1):
            value = acc[core, 2 * to + which] + arrived[to, which]
            rest = value[:, LANES:]
            packed = jnp.where(low, rest[: outs // 2], pltpu.roll(rest[outs // 2 :], width, 1))
            value = jnp.concatenate([value[:, :LANES], packed], axis=0).astype(ready.dtype)
            stays = jnp.logical_and(to == y, core == which)

            @pl.when(stays)
            def _():
                result[me] = value

            @pl.when(jnp.logical_not(stays))
            def _():
                ready[2 * to + which] = value
                remote(ready.at[2 * to + which], result.at[me], back_sem.at[0], back_sem.at[1], {"tm_0": to, "tm_1": which}).start()

    late = [(step, chunk) for step in (half - 1, half) for chunk in ORDER]
    if ny >= 8:
        events = {1: late[:1], 2: late[1:2], ny - 4: late[2:3], ny - 3: late[3:5], ny - 2: late[5:]}
    else:
        events = {1: late[:3], ny - 1: late[3:]}

    def stage(i, current, following):
        if isinstance(i, int):
            ring_events(events.get(i + 1, []))
        else:
            for k, todo in events.items():
                pl.when(i + 1 == k)(functools.partial(ring_events, todo))
        halo_wait(source(i + 1))
        prepare(source(i + 1), following)
        after(i, current)

    def after(i, current):
        src = source(i)
        totals = multiply(src, current)
        repeat_first(src, totals)
        if isinstance(i, int):
            if i > 0:
                part_copy(released(i)).start()
            if i > 1:
                finish(released(i - 1))
        else:
            pl.when(i > 0)(lambda: part_copy(released(i)).start())
            pl.when(i > 1)(lambda: finish(released(i - 1)))

    halo_wait(source(0))
    prepare(source(0), wide_a)

    @pl.loop(0, half - 1)
    def _(p):
        stage(2 * p, wide_a, wide_b)
        stage(2 * p + 1, wide_b, wide_a)

    stage(ny - 2, wide_a, wide_b)
    after(ny - 1, wide_b)
    part_copy(released(ny)).start()
    finish(released(ny - 1))
    finish(released(ny))

    several(result, tms - 1, back_sem).wait_recv()
    conv = jnp.transpose(result[:, :outs].reshape(channels, LANES).astype(jnp.float32), (1, 0))
    out[0, : rows - 1] = conv.astype(out.dtype).reshape(rows - 1, width, channels)
    rest = result[:, outs:].astype(jnp.float32)
    rest = jnp.concatenate([rest, pltpu.roll(rest, width, 2)], axis=1).reshape(channels, LANES)
    rest = jnp.transpose(rest, (1, 0))[:width]
    out[0, last] = rest.astype(out.dtype)

    for buf, n, sem in ((stat_y, tms, y_sem), (stat_z, nz, z_sem), (stat_x, nx, x_sem), (ready, tms, back_sem)):
        if n > 1:
            several(buf, n - 1, sem).wait_send()
    tap_remote.wait_send()

    def rows_out(n, sem):
        at = frames.at[pl.ds(0, n)]
        remote(at, at, sem, halo_recv.at[0], partner).wait_send()

    rows_out(rows * (2 * half - 1), ring_send)
    pl.when(inner)(lambda: rows_out(2 * ny, halo_send))
    pl.when(jnp.logical_not(inner))(lambda: rows_out(ny, halo_send))
    remote(arrived, arrived, part_send, part_recv.at[0], partner).wait_send()


def local(sizes, features, gamma, beta, kernel, bias):
    ny, nz, nx = sizes
    tms = 2 * ny
    _, rows, width, channels = features.shape
    outs = kernel.shape[1]
    taps = jnp.transpose(kernel, (0, 2, 3, 1, 4)).reshape(3, 3, 3 * outs, channels)
    wide = (rows + 1) * width
    bf16, f32 = jnp.bfloat16, jnp.float32
    dma = pltpu.SemaphoreType.DMA
    any_spec = pl.BlockSpec(memory_space=pltpu.HBM)
    vector = lambda v: v.reshape(1, channels)
    conv = pl.pallas_call(
        functools.partial(conv_kernel, sizes),
        out_shape=pltpu.VMEM(features.shape, bf16),
        in_specs=[any_spec] * 4,
        out_specs=pl.BlockSpec(memory_space=pltpu.VMEM),
        scratch_shapes=[
            pltpu.VMEM((ny * (rows + 2), width, channels), bf16),
            pltpu.VMEM((18 * outs, 3 * channels), bf16),
            pltpu.VMEM((wide, 3 * channels), bf16),
            pltpu.VMEM((wide, 3 * channels), bf16),
            pltpu.VMEM((2, tms + 2, outs, wide), f32),
            pltpu.VMEM((ny, 2, outs, wide), f32),
            pltpu.VMEM((tms, outs * 3 // 2, LANES), bf16),
            pltpu.VMEM((tms, outs * 3 // 2, LANES), bf16),
            pltpu.VMEM((2, 1, channels), f32),
            pltpu.VMEM((tms, 2, LANES), f32),
            pltpu.VMEM((nz, 2, LANES), f32),
            pltpu.VMEM((nx, 2, LANES), f32),
            pltpu.VMEM((8, channels), f32),
            dma((3,)), dma((2,)),
            dma, dma((ny, rows)),
            dma, dma((ny,)),
            dma((2,)), dma((2,)), dma((2,)),
            dma, dma((ny,)),
            dma((2,)),
        ],
        compiler_params=pltpu.CompilerParams(collective_id=0, has_side_effects=True, vmem_limit_bytes=VMEM_LIMIT),
        name="fused_block",
    )(features, vector(gamma), vector(beta), taps)
    return (features.astype(f32) + conv.astype(f32) + bias).astype(bf16)


def solution(mesh):
    sizes = (8, 8, 4)
    split = Mesh(mesh.devices.reshape(8, 2, 8, 4), TM + ROWS)
    in_specs = (P(TM, ROWS, None, None), P(), P(), P(None, TM, None, None, None), P())
    out_specs = P(TM, ROWS, None, None)
    return jax.shard_map(
        functools.partial(local, sizes), mesh=split, in_specs=in_specs, out_specs=out_specs, check_vma=False
    )
```

```python
import functools

import jax
import jax.numpy as jnp
from jax import lax
from jax.experimental import pallas as pl
from jax.experimental.pallas import tpu as pltpu
from jax.sharding import Mesh
from jax.sharding import PartitionSpec as P

GROUPS = 32
EPSILON = 1e-06
TM = ("tm_0", "tm_1")
ROWS = ("rows_0", "rows_1")
HIGHEST = lax.Precision.HIGHEST
MESH = pl.DeviceIdType.MESH
LANES = 128
VMEM_LIMIT = 67043328 - 409600
ORDER = (0, 2, 1)


def conv_kernel(
    sizes, feat, gamma, beta, kern, out,
    frames, taps, wide_a, wide_b, prod_a, prod_b, acc, arrived, ready, result, consts, stat_y, stat_z, stat_x, stat_all,
    affine, local_sem, tap_sem, ring_send, ring_recv, halo_send, halo_recv,
    y_sem, z_sem, x_sem, all_sem, part_send, part_recv, back_sem,
):
    ny, nz, nx = sizes
    tms = 2 * ny
    half = ny // 2
    rows, width, channels = feat.shape[1:]
    outs = kern.shape[2] // 3
    group = channels // GROUPS
    wide = (rows + 1) * width
    last = rows - 1
    slot = rows + 2

    y, core = lax.axis_index("tm_0"), lax.axis_index("tm_1")
    z, x = lax.axis_index("rows_0"), lax.axis_index("rows_1")
    me = 2 * y + core
    row = z * nx + x
    has_up, has_down = row > 0, row < nz * nx - 1
    inner = jnp.logical_and(has_up, has_down)

    def wrap(v, n):
        v = jnp.where(v >= n, v - n, v)
        return jnp.where(v < 0, v + n, v)

    def chip(offset):
        return wrap(y + offset, ny)

    up = {"rows_0": jnp.where(x > 0, z, wrap(z - 1, nz)), "rows_1": jnp.where(x > 0, x - 1, nx - 1)}
    down = {"rows_0": jnp.where(x < nx - 1, z, wrap(z + 1, nz)), "rows_1": jnp.where(x < nx - 1, x + 1, 0)}
    y_next, y_prev = chip(1), chip(-1)
    partner = {"tm_1": 1 - core}
    home = y * slot

    def remote(src, dst, send, recv, device):
        return pltpu.make_async_remote_copy(
            src_ref=src, dst_ref=dst, send_sem=send, recv_sem=recv,
            device_id=device, device_id_type=MESH,
        )

    own = pltpu.make_async_copy(feat.at[0], frames.at[pl.ds(home + 1, rows)], local_sem.at[0])
    own.start()

    barrier = pltpu.get_barrier_semaphore()

    def far_first(n):
        return sorted(range(1, n), key=lambda k: -min(k, n - k))

    y_peers = [{"tm_0": chip(k), "tm_1": c} for k in far_first(ny) for c in (core, 1 - core)] + [partner]
    z_peers = [{"rows_0": wrap(z + k, nz)} for k in far_first(nz)]
    x_peers = [{"rows_1": wrap(x + k, nx)} for k in far_first(nx)]

    def greet(device):
        pl.semaphore_signal(barrier, inc=1, device_id=device, device_id_type=MESH)

    for peer in y_peers + z_peers + x_peers:
        greet(peer)
    crosses_up = jnp.logical_and(has_up, x == 0)
    crosses_down = jnp.logical_and(has_down, x == nx - 1)
    expected = len(y_peers) + len(z_peers) + len(x_peers)
    if nx > 1:
        pl.when(crosses_up)(lambda: greet(up))
        pl.when(crosses_down)(lambda: greet(down))
        expected = expected + jnp.where(crosses_up, 1, 0) + jnp.where(crosses_down, 1, 0)

    for i, ref in enumerate((gamma, beta)):
        pltpu.make_async_copy(ref, consts.at[i], local_sem.at[1]).start()
    block = 3 * outs
    mine = pl.ds(pl.multiple_of(core * 3 * block, 16), 3 * block)
    for a in range(3):
        for b in range(3):
            pltpu.make_async_copy(
                kern.at[a, b],
                taps.at[pl.ds(pl.multiple_of(core * 3 * block + a * block, 16), block), pl.ds(b * channels, channels)],
                local_sem.at[2],
            ).start()

    lane = lax.broadcasted_iota(jnp.int32, (channels, LANES), 1)
    chan = lax.broadcasted_iota(jnp.int32, (channels, LANES), 0)
    member = jnp.where(chan // group == lane, 1.0, 0.0)

    def gather_groups(v):
        return lax.dot_general(v, member, (((1,), (0,)), ((), ())), precision=HIGHEST, preferred_element_type=jnp.float32)

    def spread_groups(v):
        return lax.dot_general(v, member, (((1,), (1,)), ((), ())), precision=HIGHEST, preferred_element_type=jnp.float32)

    acc[...] = jnp.zeros_like(acc)
    for unfolded in (wide_a, wide_b):
        unfolded[rows * width :, :] = jnp.zeros((width, 3 * channels), unfolded.dtype)

    own.wait()
    count = rows * width
    values = frames[pl.ds(home + 1, rows)].reshape(count, channels).astype(jnp.float32)
    mean_c = jnp.sum(values, axis=0, keepdims=True) * (1.0 / count)
    off = values - mean_c
    m2_c = jnp.sum(off * off, axis=0, keepdims=True)
    mean_c8 = jnp.broadcast_to(mean_c, (8, channels))
    mean_g = gather_groups(mean_c8) * (1.0 / group)
    apart = mean_c8 - spread_groups(mean_g)
    m2_g = gather_groups(m2_c + count * (apart * apart))
    stat_y[me] = jnp.concatenate([mean_g[0:1], m2_g[0:1]], axis=0)

    pl.semaphore_wait(barrier, expected)

    def publish(buf, at, peers, sem):
        for peer in peers:
            remote(buf.at[at], buf.at[at], sem.at[0], sem.at[1], peer).start()

    def several(buf, n, sem):
        return remote(buf.at[pl.ds(0, n)], buf.at[pl.ds(0, n)], sem.at[0], sem.at[1], partner)

    def collect(buf, peers, sem, weight):
        if peers:
            several(buf, len(peers), sem).wait_recv()
        means, m2s = buf[:, 0:1, :], buf[:, 1:2, :]
        mean = jnp.sum(means, axis=0) * (1.0 / buf.shape[0])
        gap = means - mean[None]
        m2 = jnp.sum(m2s, axis=0) + weight * jnp.sum(gap * gap, axis=0)
        return jnp.concatenate([mean, m2], axis=0)

    publish(stat_y, me, y_peers, y_sem)

    def ring_copy(src, way, chunk):
        at = frames.at[src * slot + 1 + chunk]
        return remote(at, at, ring_send, ring_recv.at[src, chunk], {"tm_0": y_next if way == 0 else y_prev})

    def halo_copy(src, side):
        at, to = (1, rows + 1) if side == 0 else (rows, 0)
        return remote(
            frames.at[src * slot + at], frames.at[src * slot + to], halo_send, halo_recv.at[src], up if side == 0 else down
        )

    def send_halo(src, chunk):
        if chunk == 0:
            pl.when(has_up)(lambda: halo_copy(src, 0).start())
        if chunk == last:
            pl.when(has_down)(lambda: halo_copy(src, 1).start())

    for chunk in ORDER:
        ring_copy(y, 0, chunk).start()
        ring_copy(y, 1, chunk).start()
    for chunk in (0, last):
        send_halo(y, chunk)

    pltpu.make_async_copy(taps.at[mine], taps.at[mine], local_sem.at[2]).wait()
    tap_remote = remote(taps.at[mine], taps.at[mine], tap_sem.at[0], tap_sem.at[1], partner)
    tap_remote.start()
    pltpu.make_async_copy(consts, consts, local_sem.at[1]).wait()

    def ring_event(step, chunk):
        for way in (0, 1):
            src = chip(-step) if way == 0 else chip(step)

            def arrive(src=src, way=way):
                ring_copy(src, way, chunk).wait_recv()
                if step < half - 1:
                    ring_copy(src, way, chunk).start()
                elif step == half - 1:
                    pl.when(core == way)(lambda: ring_copy(src, way, chunk).start())
                send_halo(src, chunk)

            if step < half:
                arrive()
            else:
                pl.when(core == way)(arrive)

    per_device = float(rows * width * group)
    early = [(step, chunk) for step in range(1, half - 1) for chunk in ORDER]

    def ring_events(todo):
        for step, chunk in todo:
            ring_event(step, chunk)

    ring_events(early[:1])
    lead = core == 1
    span = collect(stat_y, y_peers, y_sem, per_device)

    @pl.when(lead)
    def _():
        stat_z[z] = span
        publish(stat_z, z, z_peers, z_sem)

    ring_events(early[1:4])

    @pl.when(lead)
    def _():
        stat_x[x] = collect(stat_z, z_peers, z_sem, per_device * tms)
        publish(stat_x, x, x_peers, x_sem)

    ring_events(early[4:])
    hand_over = remote(stat_all, stat_all, all_sem.at[0], all_sem.at[1], partner)

    @pl.when(lead)
    def _():
        stat_all[...] = collect(stat_x, x_peers, x_sem, per_device * tms * nz)
        hand_over.start()

    @pl.when(jnp.logical_not(lead))
    def _():
        hand_over.wait_recv()

    final = stat_all[...]
    total = per_device * tms * nz * nx
    inv = lax.rsqrt(final[1:2] * (1.0 / total) + EPSILON)
    both = spread_groups(jnp.concatenate([final[0:1], inv] + [jnp.zeros((6, LANES), jnp.float32)], axis=0))
    affine[0:1] = both[0:1]
    affine[1:2] = 0.5 * both[1:2] * consts[0]
    affine[2:3] = 0.5 * consts[1]
    tap_remote.wait_recv()

    column = lax.rem(lax.broadcasted_iota(jnp.int32, (outs, wide), 1), width)
    at_left, at_right = column == 0, column == width - 1

    def source(k):
        if isinstance(k, int):
            return chip((k + 1) // 2 if k % 2 else -(k // 2))
        return chip(jnp.where(lax.rem(k, 2) == 1, (k + 1) // 2, -(k // 2)))

    def halo_wait(src):
        def rows_in(n):
            at = frames.at[pl.ds(0, n)]
            remote(at, at, halo_send, halo_recv.at[src], partner).wait_recv()

        pl.when(inner)(lambda: rows_in(2))
        pl.when(jnp.logical_not(inner))(lambda: rows_in(1))

    def prepare(src, unfolded):
        for r in range(rows + 2):
            value = frames[src * slot + r].astype(jnp.float32)
            h = (value - affine[0:1]) * affine[1:2] + affine[2:3]
            active = h + h * jnp.tanh(h)
            if r == 0:
                active = jnp.where(has_up, active, 0.0)
            if r == rows + 1:
                active = jnp.where(has_down, active, 0.0)
            active = active.astype(unfolded.dtype)
            for b in range(3):
                if 0 <= r - b < rows:
                    unfolded[(r - b) * width : (r - b + 1) * width, b * channels : (b + 1) * channels] = active

    def multiply(unfolded, product):
        for owner in (0, 1):
            part = slice(owner * 3 * block, (owner + 1) * 3 * block)
            product[part] = lax.dot_general(
                taps[part], unfolded[...], (((1,), (1,)), ((), ())), preferred_element_type=jnp.float32
            )

    def accumulate(src, product):
        frame = 2 * src + core
        totals = []
        for owner in (0, 1):
            for a in range(3):
                base = (owner * 3 + a) * block
                one, two, three = (product[base + c * outs : base + (c + 1) * outs] for c in range(3))
                one = jnp.where(at_left, 0.0, pltpu.roll(one, 1, 1))
                three = jnp.where(at_right, 0.0, pltpu.roll(three, wide - 1, 1))
                total = one + two + three
                acc[owner, frame + 2 - a] += total
                totals.append(total)
        return totals

    def repeat_first(src, totals):
        @pl.when(2 * src + core == 0)
        def _():
            for owner in (0, 1):
                acc[owner, 0] += totals[3 * owner] + totals[3 * owner + 1]
                acc[owner, 1] += totals[3 * owner]

    def released(j):
        if isinstance(j, int):
            return chip((j + 1) // 2 if j % 2 else 1 - j // 2)
        return chip(jnp.where(lax.rem(j, 2) == 1, (j + 1) // 2, 1 - j // 2))

    def part_copy(to):
        return remote(acc.at[1 - core, pl.ds(2 * to, 2)], arrived.at[to], part_send, part_recv.at[to], partner)

    low = lax.broadcasted_iota(jnp.int32, (outs // 2, LANES), 1) < width

    def finish(to):
        part_copy(to).wait_recv()
        for which in (0, 1):
            value = acc[core, 2 * to + which] + arrived[to, which]
            rest = value[:, LANES:]
            packed = jnp.where(low, rest[: outs // 2], pltpu.roll(rest[outs // 2 :], width, 1))
            value = jnp.concatenate([value[:, :LANES], packed], axis=0).astype(ready.dtype)
            stays = jnp.logical_and(to == y, core == which)

            @pl.when(stays)
            def _():
                result[me] = value

            @pl.when(jnp.logical_not(stays))
            def _():
                ready[2 * to + which] = value
                remote(ready.at[2 * to + which], result.at[me], back_sem.at[0], back_sem.at[1], {"tm_0": to, "tm_1": which}).start()

    late = [(step, chunk) for step in (half - 1, half) for chunk in ORDER]
    if ny >= 8:
        events = {1: late[:1], 2: late[1:2], 3: late[2:3], 4: late[3:4], 5: late[4:5], ny - 1: late[5:]}
    else:
        events = {1: late[:3], ny - 1: late[3:]}
    wides, prods = (wide_a, wide_b), (prod_a, prod_b)

    def arrivals(k):
        if isinstance(k, int):
            ring_events(events.get(k, []))
        else:
            for when, todo in events.items():
                pl.when(k == when)(functools.partial(ring_events, todo))
        halo_wait(source(k))

    def stage(i, parity):
        other = 1 - parity
        arrivals(i + 1)
        prepare(source(i + 1), wides[other])
        multiply(wides[parity], prods[parity])
        sums(i - 1, other)
        pl.when(i > 1)(lambda: part_copy(released(i - 1)).start())
        pl.when(i > 2)(lambda: finish(released(i - 2)))

    def sums(i, parity):
        repeat_first(source(i), accumulate(source(i), prods[parity]))

    arrivals(0)
    prepare(source(0), wide_a)
    arrivals(1)
    prepare(source(1), wide_b)
    multiply(wide_a, prod_a)

    @pl.loop(0, half - 2)
    def _(p):
        stage(2 * p + 1, 1)
        stage(2 * p + 2, 0)

    stage(ny - 3, 1)
    multiply(wide_a, prod_a)
    sums(ny - 3, 1)
    part_copy(released(ny - 3)).start()
    if ny > 4:
        finish(released(ny - 4))
    sums(ny - 2, 0)
    part_copy(released(ny - 2)).start()
    arrivals(ny - 1)
    finish(released(ny - 3))
    prepare(source(ny - 1), wide_b)
    multiply(wide_b, prod_b)
    sums(ny - 1, 1)
    part_copy(released(ny - 1)).start()
    part_copy(released(ny)).start()
    for j in range(ny - 2, ny + 1):
        finish(released(j))

    several(result, tms - 1, back_sem).wait_recv()
    conv = jnp.transpose(result[:, :outs].reshape(channels, LANES).astype(jnp.float32), (1, 0))
    out[0, : rows - 1] = conv.astype(out.dtype).reshape(rows - 1, width, channels)
    rest = result[:, outs:].astype(jnp.float32)
    rest = jnp.concatenate([rest, pltpu.roll(rest, width, 2)], axis=1).reshape(channels, LANES)
    rest = jnp.transpose(rest, (1, 0))[:width]
    out[0, last] = rest.astype(out.dtype)

    several(stat_y, tms - 1, y_sem).wait_send()
    several(ready, tms - 1, back_sem).wait_send()

    @pl.when(lead)
    def _():
        for buf, n, sem in ((stat_z, nz, z_sem), (stat_x, nx, x_sem)):
            if n > 1:
                several(buf, n - 1, sem).wait_send()
        hand_over.wait_send()

    tap_remote.wait_send()

    def rows_out(n, sem):
        at = frames.at[pl.ds(0, n)]
        remote(at, at, sem, halo_recv.at[0], partner).wait_send()

    rows_out(rows * (2 * half - 1), ring_send)
    pl.when(inner)(lambda: rows_out(2 * ny, halo_send))
    pl.when(jnp.logical_not(inner))(lambda: rows_out(ny, halo_send))
    remote(arrived, arrived, part_send, part_recv.at[0], partner).wait_send()


def local(sizes, features, gamma, beta, kernel, bias):
    ny, nz, nx = sizes
    tms = 2 * ny
    _, rows, width, channels = features.shape
    outs = kernel.shape[1]
    taps = jnp.transpose(kernel, (0, 2, 3, 1, 4)).reshape(3, 3, 3 * outs, channels)
    wide = (rows + 1) * width
    bf16, f32 = jnp.bfloat16, jnp.float32
    dma = pltpu.SemaphoreType.DMA
    any_spec = pl.BlockSpec(memory_space=pltpu.HBM)
    vector = lambda v: v.reshape(1, channels)
    conv = pl.pallas_call(
        functools.partial(conv_kernel, sizes),
        out_shape=pltpu.VMEM(features.shape, bf16),
        in_specs=[any_spec] * 4,
        out_specs=pl.BlockSpec(memory_space=pltpu.VMEM),
        scratch_shapes=[
            pltpu.VMEM((ny * (rows + 2), width, channels), bf16),
            pltpu.VMEM((18 * outs, 3 * channels), bf16),
            pltpu.VMEM((wide, 3 * channels), bf16),
            pltpu.VMEM((wide, 3 * channels), bf16),
            pltpu.VMEM((18 * outs, wide), f32),
            pltpu.VMEM((18 * outs, wide), f32),
            pltpu.VMEM((2, tms + 2, outs, wide), f32),
            pltpu.VMEM((ny, 2, outs, wide), f32),
            pltpu.VMEM((tms, outs * 3 // 2, LANES), bf16),
            pltpu.VMEM((tms, outs * 3 // 2, LANES), bf16),
            pltpu.VMEM((2, 1, channels), f32),
            pltpu.VMEM((tms, 2, LANES), f32),
            pltpu.VMEM((nz, 2, LANES), f32),
            pltpu.VMEM((nx, 2, LANES), f32),
            pltpu.VMEM((2, LANES), f32),
            pltpu.VMEM((8, channels), f32),
            dma((3,)), dma((2,)),
            dma, dma((ny, rows)),
            dma, dma((ny,)),
            dma((2,)), dma((2,)), dma((2,)), dma((2,)),
            dma, dma((ny,)),
            dma((2,)),
        ],
        compiler_params=pltpu.CompilerParams(collective_id=0, has_side_effects=True, vmem_limit_bytes=VMEM_LIMIT),
        name="fused_block",
    )(features, vector(gamma), vector(beta), taps)
    return (features.astype(f32) + conv.astype(f32) + bias).astype(bf16)


def solution(mesh):
    sizes = (8, 8, 4)
    split = Mesh(mesh.devices.reshape(8, 2, 8, 4), TM + ROWS)
    in_specs = (P(TM, ROWS, None, None), P(), P(), P(None, TM, None, None, None), P())
    out_specs = P(TM, ROWS, None, None)
    return jax.shard_map(
        functools.partial(local, sizes), mesh=split, in_specs=in_specs, out_specs=out_specs, check_vma=False
    )
```

```python
import functools

import jax
import jax.numpy as jnp
from jax import lax
from jax.experimental import pallas as pl
from jax.experimental.pallas import tpu as pltpu
from jax.sharding import Mesh
from jax.sharding import PartitionSpec as P

GROUPS = 32
EPSILON = 1e-06
TM = ("tm_0", "tm_1")
ROWS = ("rows_0", "rows_1")
HIGHEST = lax.Precision.HIGHEST
MESH = pl.DeviceIdType.MESH
LANES = 128
HEAD = 2
PLAN = {1: (0, 1, 2), 2: (3,), 3: (4,), 7: (5,)}
VMEM_LIMIT = 67043328 - 409600
ORDER = (0, 2, 1)


def conv_kernel(
    sizes, feat, gamma, beta, kern, out,
    frames, taps, wide_a, wide_b, prod_a, prod_b, acc, arrived, ready, result, consts, stat_y, stat_z, stat_x, stat_all,
    affine, local_sem, tap_sem, ring_send, ring_recv, halo_send, halo_recv,
    z_in, y_sem, z_sem, x_sem, all_sem, part_send, part_recv, back_sem,
):
    ny, nz, nx = sizes
    tms = 2 * ny
    half = ny // 2
    rows, width, channels = feat.shape[1:]
    outs = kern.shape[2] // 3
    group = channels // GROUPS
    wide = (rows + 1) * width
    last = rows - 1
    slot = rows + 2

    y, core = lax.axis_index("tm_0"), lax.axis_index("tm_1")
    z, x = lax.axis_index("rows_0"), lax.axis_index("rows_1")
    me = 2 * y + core
    row = z * nx + x
    has_up, has_down = row > 0, row < nz * nx - 1
    inner = jnp.logical_and(has_up, has_down)

    def wrap(v, n):
        v = jnp.where(v >= n, v - n, v)
        return jnp.where(v < 0, v + n, v)

    def chip(offset):
        return wrap(y + offset, ny)

    up = {"rows_0": jnp.where(x > 0, z, wrap(z - 1, nz)), "rows_1": jnp.where(x > 0, x - 1, nx - 1)}
    down = {"rows_0": jnp.where(x < nx - 1, z, wrap(z + 1, nz)), "rows_1": jnp.where(x < nx - 1, x + 1, 0)}
    y_next, y_prev = chip(1), chip(-1)
    partner = {"tm_1": 1 - core}
    home = y * slot

    def remote(src, dst, send, recv, device):
        return pltpu.make_async_remote_copy(
            src_ref=src, dst_ref=dst, send_sem=send, recv_sem=recv,
            device_id=device, device_id_type=MESH,
        )

    own = pltpu.make_async_copy(feat.at[0], frames.at[pl.ds(home + 1, rows)], local_sem.at[0])
    own.start()

    barrier = pltpu.get_barrier_semaphore()

    def far_first(n):
        return sorted(range(1, n), key=lambda k: -min(k, n - k))

    y_peers = [{"tm_0": chip(k), "tm_1": c} for k in far_first(ny) for c in (core, 1 - core)] + [partner]
    z_peers = [{"rows_0": wrap(z + k, nz)} for k in far_first(nz)]
    x_peers = [{"rows_1": wrap(x + k, nx)} for k in far_first(nx)]

    def greet(device):
        pl.semaphore_signal(barrier, inc=1, device_id=device, device_id_type=MESH)

    lead = core == 1
    for k in far_first(nz):
        pl.when(jnp.logical_and(lead, z + k < nz))(functools.partial(greet, {"rows_0": z + k}))
    for peer in y_peers + x_peers:
        greet(peer)
    crosses_up = jnp.logical_and(has_up, x == 0)
    crosses_down = jnp.logical_and(has_down, x == nx - 1)
    expected = len(y_peers) + len(x_peers) + jnp.where(lead, z, 0)
    if nx > 1:
        pl.when(crosses_up)(lambda: greet(up))
        pl.when(crosses_down)(lambda: greet(down))
        expected = expected + jnp.where(crosses_up, 1, 0) + jnp.where(crosses_down, 1, 0)

    for i, ref in enumerate((gamma, beta)):
        pltpu.make_async_copy(ref, consts.at[i], local_sem.at[1]).start()
    block = 3 * outs
    mine = pl.ds(pl.multiple_of(core * 3 * block, 16), 3 * block)
    for a in range(3):
        for b in range(3):
            pltpu.make_async_copy(
                kern.at[a, b],
                taps.at[pl.ds(pl.multiple_of(core * 3 * block + a * block, 16), block), pl.ds(b * channels, channels)],
                local_sem.at[2],
            ).start()

    lane = lax.broadcasted_iota(jnp.int32, (channels, LANES), 1)
    chan = lax.broadcasted_iota(jnp.int32, (channels, LANES), 0)
    member = jnp.where(chan // group == lane, 1.0, 0.0)

    def gather_groups(v):
        return lax.dot_general(v, member, (((1,), (0,)), ((), ())), precision=HIGHEST, preferred_element_type=jnp.float32)

    def spread_groups(v):
        return lax.dot_general(v, member, (((1,), (1,)), ((), ())), precision=HIGHEST, preferred_element_type=jnp.float32)

    acc[...] = jnp.zeros_like(acc)
    for unfolded in (wide_a, wide_b):
        unfolded[rows * width :, :] = jnp.zeros((width, 3 * channels), unfolded.dtype)

    own.wait()
    count = rows * width
    values = frames[pl.ds(home + 1, rows)].reshape(count, channels).astype(jnp.float32)
    mean_c = jnp.sum(values, axis=0, keepdims=True) * (1.0 / count)
    off = values - mean_c
    m2_c = jnp.sum(off * off, axis=0, keepdims=True)
    mean_c8 = jnp.broadcast_to(mean_c, (8, channels))
    mean_g = gather_groups(mean_c8) * (1.0 / group)
    apart = mean_c8 - spread_groups(mean_g)
    m2_g = gather_groups(m2_c + count * (apart * apart))
    stat_y[me] = jnp.concatenate([mean_g[0:1], m2_g[0:1]], axis=0)

    pl.semaphore_wait(barrier, expected)
    for k in far_first(nz):

        @pl.when(jnp.logical_and(lead, z - k >= 0))
        def _():
            pl.semaphore_signal(z_in, inc=1, device_id={"rows_0": z - k}, device_id_type=MESH)


    def publish(buf, at, peers, sem):
        for peer in peers:
            remote(buf.at[at], buf.at[at], sem.at[0], sem.at[1], peer).start()

    def several(buf, n, sem):
        return remote(buf.at[pl.ds(0, n)], buf.at[pl.ds(0, n)], sem.at[0], sem.at[1], partner)

    def collect(buf, peers, sem, weight):
        if peers:
            several(buf, len(peers), sem).wait_recv()
        means, m2s = buf[:, 0:1, :], buf[:, 1:2, :]
        mean = jnp.sum(means, axis=0) * (1.0 / buf.shape[0])
        gap = means - mean[None]
        m2 = jnp.sum(m2s, axis=0) + weight * jnp.sum(gap * gap, axis=0)
        return jnp.concatenate([mean, m2], axis=0)

    publish(stat_y, me, y_peers, y_sem)

    def ring_copy(src, way, chunk):
        at = frames.at[src * slot + 1 + chunk]
        return remote(at, at, ring_send, ring_recv.at[src, chunk], {"tm_0": y_next if way == 0 else y_prev})

    def halo_copy(src, side):
        at, to = (1, rows + 1) if side == 0 else (rows, 0)
        return remote(
            frames.at[src * slot + at], frames.at[src * slot + to], halo_send, halo_recv.at[src], up if side == 0 else down
        )

    def send_halo(src, chunk):
        if chunk == 0:
            pl.when(has_up)(lambda: halo_copy(src, 0).start())
        if chunk == last:
            pl.when(has_down)(lambda: halo_copy(src, 1).start())

    for chunk in ORDER:
        ring_copy(y, 0, chunk).start()
        ring_copy(y, 1, chunk).start()
    for chunk in (0, last):
        send_halo(y, chunk)

    pltpu.make_async_copy(taps.at[mine], taps.at[mine], local_sem.at[2]).wait()
    tap_remote = remote(taps.at[mine], taps.at[mine], tap_sem.at[0], tap_sem.at[1], partner)
    tap_remote.start()
    pltpu.make_async_copy(consts, consts, local_sem.at[1]).wait()

    def ring_event(step, chunk):
        for way in (0, 1):
            src = chip(-step) if way == 0 else chip(step)

            def arrive(src=src, way=way):
                ring_copy(src, way, chunk).wait_recv()
                if step < half - 1:
                    ring_copy(src, way, chunk).start()
                elif step == half - 1:
                    pl.when(core == way)(lambda: ring_copy(src, way, chunk).start())
                send_halo(src, chunk)

            if step < half:
                arrive()
            else:
                pl.when(core == way)(arrive)

    per_device = float(rows * width * group)
    early = [(step, chunk) for step in range(1, half - 1) for chunk in ORDER]

    def ring_events(todo):
        for step, chunk in todo:
            ring_event(step, chunk)

    ring_events(early[:1])
    span = collect(stat_y, y_peers, y_sem, per_device)

    @pl.when(lead)
    def _():
        stat_z[z] = span
        pl.when(z < nz - 1)(lambda: pl.semaphore_wait(z_in, nz - 1 - z))
        publish(stat_z, z, z_peers, z_sem)

    ring_events(early[1:4])

    @pl.when(lead)
    def _():
        stat_x[x] = collect(stat_z, z_peers, z_sem, per_device * tms)
        publish(stat_x, x, x_peers, x_sem)

    late = [(step, chunk) for step in (half - 1, half) for chunk in ORDER]
    ring_events(early[4:] + late[: HEAD if ny >= 8 else 0])
    hand_over = remote(stat_all, stat_all, all_sem.at[0], all_sem.at[1], partner)

    @pl.when(lead)
    def _():
        stat_all[...] = collect(stat_x, x_peers, x_sem, per_device * tms * nz)
        hand_over.start()

    @pl.when(jnp.logical_not(lead))
    def _():
        hand_over.wait_recv()

    final = stat_all[...]
    total = per_device * tms * nz * nx
    inv = lax.rsqrt(final[1:2] * (1.0 / total) + EPSILON)
    both = spread_groups(jnp.concatenate([final[0:1], inv] + [jnp.zeros((6, LANES), jnp.float32)], axis=0))
    affine[0:1] = both[0:1]
    affine[1:2] = 0.5 * both[1:2] * consts[0]
    affine[2:3] = 0.5 * consts[1]
    tap_remote.wait_recv()

    column = lax.rem(lax.broadcasted_iota(jnp.int32, (outs, wide), 1), width)
    at_left, at_right = column == 0, column == width - 1

    def source(k):
        if isinstance(k, int):
            return chip((k + 1) // 2 if k % 2 else -(k // 2))
        return chip(jnp.where(lax.rem(k, 2) == 1, (k + 1) // 2, -(k // 2)))

    def halo_wait(src):
        def rows_in(n):
            at = frames.at[pl.ds(0, n)]
            remote(at, at, halo_send, halo_recv.at[src], partner).wait_recv()

        pl.when(inner)(lambda: rows_in(2))
        pl.when(jnp.logical_not(inner))(lambda: rows_in(1))

    def prepare(src, unfolded):
        for r in range(rows + 2):
            value = frames[src * slot + r].astype(jnp.float32)
            h = (value - affine[0:1]) * affine[1:2] + affine[2:3]
            active = h + h * jnp.tanh(h)
            if r == 0:
                active = jnp.where(has_up, active, 0.0)
            if r == rows + 1:
                active = jnp.where(has_down, active, 0.0)
            active = active.astype(unfolded.dtype)
            for b in range(3):
                if 0 <= r - b < rows:
                    unfolded[(r - b) * width : (r - b + 1) * width, b * channels : (b + 1) * channels] = active

    def multiply(unfolded, product):
        for owner in (0, 1):
            part = slice(owner * 3 * block, (owner + 1) * 3 * block)
            product[part] = lax.dot_general(
                taps[part], unfolded[...], (((1,), (1,)), ((), ())), preferred_element_type=jnp.float32
            )

    def accumulate(src, product):
        frame = 2 * src + core
        totals = []
        for owner in (0, 1):
            for a in range(3):
                base = (owner * 3 + a) * block
                one, two, three = (product[base + c * outs : base + (c + 1) * outs] for c in range(3))
                one = jnp.where(at_left, 0.0, pltpu.roll(one, 1, 1))
                three = jnp.where(at_right, 0.0, pltpu.roll(three, wide - 1, 1))
                total = one + two + three
                acc[owner, frame + 2 - a] += total
                totals.append(total)
        return totals

    def repeat_first(src, totals):
        @pl.when(2 * src + core == 0)
        def _():
            for owner in (0, 1):
                acc[owner, 0] += totals[3 * owner] + totals[3 * owner + 1]
                acc[owner, 1] += totals[3 * owner]

    def released(j):
        if isinstance(j, int):
            return chip((j + 1) // 2 if j % 2 else 1 - j // 2)
        return chip(jnp.where(lax.rem(j, 2) == 1, (j + 1) // 2, 1 - j // 2))

    def part_copy(to):
        return remote(acc.at[1 - core, pl.ds(2 * to, 2)], arrived.at[to], part_send, part_recv.at[to], partner)

    low = lax.broadcasted_iota(jnp.int32, (outs // 2, LANES), 1) < width

    def finish(to):
        part_copy(to).wait_recv()
        for which in (0, 1):
            value = acc[core, 2 * to + which] + arrived[to, which]
            rest = value[:, LANES:]
            packed = jnp.where(low, rest[: outs // 2], pltpu.roll(rest[outs // 2 :], width, 1))
            value = jnp.concatenate([value[:, :LANES], packed], axis=0).astype(ready.dtype)
            stays = jnp.logical_and(to == y, core == which)

            @pl.when(stays)
            def _():
                result[me] = value

            @pl.when(jnp.logical_not(stays))
            def _():
                ready[2 * to + which] = value
                remote(ready.at[2 * to + which], result.at[me], back_sem.at[0], back_sem.at[1], {"tm_0": to, "tm_1": which}).start()

    if ny >= 8:
        events = {k: [late[e] for e in todo if e >= HEAD] for k, todo in PLAN.items()}
        events = {k: todo for k, todo in events.items() if todo}
    else:
        events = {1: late[:3], ny - 1: late[3:]}
    wides, prods = (wide_a, wide_b), (prod_a, prod_b)

    def arrivals(k):
        if isinstance(k, int):
            ring_events(events.get(k, []))
        else:
            for when, todo in events.items():
                pl.when(k == when)(functools.partial(ring_events, todo))
        halo_wait(source(k))

    def stage(i, parity):
        other = 1 - parity
        arrivals(i + 1)
        prepare(source(i + 1), wides[other])
        multiply(wides[parity], prods[parity])
        sums(i - 1, other)
        pl.when(i > 1)(lambda: part_copy(released(i - 1)).start())
        pl.when(i > 2)(lambda: finish(released(i - 2)))

    def sums(i, parity):
        repeat_first(source(i), accumulate(source(i), prods[parity]))

    arrivals(0)
    prepare(source(0), wide_a)
    arrivals(1)
    prepare(source(1), wide_b)
    multiply(wide_a, prod_a)

    @pl.loop(0, half - 2)
    def _(p):
        stage(2 * p + 1, 1)
        stage(2 * p + 2, 0)

    stage(ny - 3, 1)
    multiply(wide_a, prod_a)
    sums(ny - 3, 1)
    part_copy(released(ny - 3)).start()
    if ny > 4:
        finish(released(ny - 4))
    sums(ny - 2, 0)
    part_copy(released(ny - 2)).start()
    arrivals(ny - 1)
    prepare(source(ny - 1), wide_b)
    multiply(wide_b, prod_b)
    finish(released(ny - 3))
    sums(ny - 1, 1)
    part_copy(released(ny - 1)).start()
    part_copy(released(ny)).start()
    for j in range(ny - 2, ny + 1):
        finish(released(j))

    several(result, tms - 1, back_sem).wait_recv()
    conv = jnp.transpose(result[:, :outs].reshape(channels, LANES).astype(jnp.float32), (1, 0))
    out[0, : rows - 1] = conv.astype(out.dtype).reshape(rows - 1, width, channels)
    rest = result[:, outs:].astype(jnp.float32)
    rest = jnp.concatenate([rest, pltpu.roll(rest, width, 2)], axis=1).reshape(channels, LANES)
    rest = jnp.transpose(rest, (1, 0))[:width]
    out[0, last] = rest.astype(out.dtype)

    several(stat_y, tms - 1, y_sem).wait_send()
    several(ready, tms - 1, back_sem).wait_send()

    @pl.when(lead)
    def _():
        for buf, n, sem in ((stat_z, nz, z_sem), (stat_x, nx, x_sem)):
            if n > 1:
                several(buf, n - 1, sem).wait_send()
        hand_over.wait_send()

    tap_remote.wait_send()

    def rows_out(n, sem):
        at = frames.at[pl.ds(0, n)]
        remote(at, at, sem, halo_recv.at[0], partner).wait_send()

    rows_out(rows * (2 * half - 1), ring_send)
    pl.when(inner)(lambda: rows_out(2 * ny, halo_send))
    pl.when(jnp.logical_not(inner))(lambda: rows_out(ny, halo_send))
    remote(arrived, arrived, part_send, part_recv.at[0], partner).wait_send()


def local(sizes, features, gamma, beta, kernel, bias):
    ny, nz, nx = sizes
    tms = 2 * ny
    _, rows, width, channels = features.shape
    outs = kernel.shape[1]
    taps = jnp.transpose(kernel, (0, 2, 3, 1, 4)).reshape(3, 3, 3 * outs, channels)
    wide = (rows + 1) * width
    bf16, f32 = jnp.bfloat16, jnp.float32
    dma = pltpu.SemaphoreType.DMA
    any_spec = pl.BlockSpec(memory_space=pltpu.HBM)
    vector = lambda v: v.reshape(1, channels)
    conv = pl.pallas_call(
        functools.partial(conv_kernel, sizes),
        out_shape=pltpu.VMEM(features.shape, bf16),
        in_specs=[any_spec] * 4,
        out_specs=pl.BlockSpec(memory_space=pltpu.VMEM),
        scratch_shapes=[
            pltpu.VMEM((ny * (rows + 2), width, channels), bf16),
            pltpu.VMEM((18 * outs, 3 * channels), bf16),
            pltpu.VMEM((wide, 3 * channels), bf16),
            pltpu.VMEM((wide, 3 * channels), bf16),
            pltpu.VMEM((18 * outs, wide), f32),
            pltpu.VMEM((18 * outs, wide), f32),
            pltpu.VMEM((2, tms + 2, outs, wide), f32),
            pltpu.VMEM((ny, 2, outs, wide), f32),
            pltpu.VMEM((tms, outs * 3 // 2, LANES), bf16),
            pltpu.VMEM((tms, outs * 3 // 2, LANES), bf16),
            pltpu.VMEM((2, 1, channels), f32),
            pltpu.VMEM((tms, 2, LANES), f32),
            pltpu.VMEM((nz, 2, LANES), f32),
            pltpu.VMEM((nx, 2, LANES), f32),
            pltpu.VMEM((2, LANES), f32),
            pltpu.VMEM((8, channels), f32),
            dma((3,)), dma((2,)),
            dma, dma((ny, rows)),
            dma, dma((ny,)),
            pltpu.SemaphoreType.REGULAR,
            dma((2,)), dma((2,)), dma((2,)), dma((2,)),
            dma, dma((ny,)),
            dma((2,)),
        ],
        compiler_params=pltpu.CompilerParams(collective_id=0, has_side_effects=True, vmem_limit_bytes=VMEM_LIMIT),
        name="fused_block",
    )(features, vector(gamma), vector(beta), taps)
    return (features.astype(f32) + conv.astype(f32) + bias).astype(bf16)


def solution(mesh):
    sizes = (8, 8, 4)
    split = Mesh(mesh.devices.reshape(8, 2, 8, 4), TM + ROWS)
    in_specs = (P(TM, ROWS, None, None), P(), P(), P(None, TM, None, None, None), P())
    out_specs = P(TM, ROWS, None, None)
    return jax.shard_map(
        functools.partial(local, sizes), mesh=split, in_specs=in_specs, out_specs=out_specs, check_vma=False
    )
```

```python
import functools

import jax
import jax.numpy as jnp
from jax import lax
from jax.experimental import pallas as pl
from jax.experimental.pallas import tpu as pltpu
from jax.sharding import Mesh
from jax.sharding import PartitionSpec as P

GROUPS = 32
EPSILON = 1e-06
TM = ("tm_0", "tm_1")
ROWS = ("rows_0", "rows_1")
HIGHEST = lax.Precision.HIGHEST
MESH = pl.DeviceIdType.MESH
LANES = 128
HEAD = 2
PLAN = {1: (0, 1, 2), 2: (3,), 3: (4,), 7: (5,)}
VMEM_LIMIT = 67043328 - 409600
ORDER = (0, 2, 1)


def conv_kernel(
    sizes, feat, gamma, beta, kern, out,
    frames, taps, wide_a, wide_b, prod_a, prod_b, acc, arrived, ready, result, consts, stat_y, stat_z, stat_x,
    affine, local_sem, tap_sem, ring_send, ring_recv, halo_send, halo_recv,
    z_in, y_sem, z_sem, x_sem, part_send, part_recv, back_sem,
):
    ny, nz, nx = sizes
    tms = 2 * ny
    half = ny // 2
    rows, width, channels = feat.shape[1:]
    outs = kern.shape[2] // 3
    group = channels // GROUPS
    wide = (rows + 1) * width
    last = rows - 1
    slot = rows + 2

    y, core = lax.axis_index("tm_0"), lax.axis_index("tm_1")
    z, x = lax.axis_index("rows_0"), lax.axis_index("rows_1")
    me = 2 * y + core
    row = z * nx + x
    has_up, has_down = row > 0, row < nz * nx - 1
    inner = jnp.logical_and(has_up, has_down)

    def wrap(v, n):
        v = jnp.where(v >= n, v - n, v)
        return jnp.where(v < 0, v + n, v)

    def chip(offset):
        return wrap(y + offset, ny)

    up = {"rows_0": jnp.where(x > 0, z, wrap(z - 1, nz)), "rows_1": jnp.where(x > 0, x - 1, nx - 1)}
    down = {"rows_0": jnp.where(x < nx - 1, z, wrap(z + 1, nz)), "rows_1": jnp.where(x < nx - 1, x + 1, 0)}
    y_next, y_prev = chip(1), chip(-1)
    partner = {"tm_1": 1 - core}
    home = y * slot

    def remote(src, dst, send, recv, device):
        return pltpu.make_async_remote_copy(
            src_ref=src, dst_ref=dst, send_sem=send, recv_sem=recv,
            device_id=device, device_id_type=MESH,
        )

    own = pltpu.make_async_copy(feat.at[0], frames.at[pl.ds(home + 1, rows)], local_sem.at[0])
    own.start()

    barrier = pltpu.get_barrier_semaphore()

    def far_first(n):
        return sorted(range(1, n), key=lambda k: -min(k, n - k))

    y_peers = [{"tm_0": chip(k), "tm_1": c} for k in far_first(ny) for c in (core, 1 - core)] + [partner]
    z_peers = [{"rows_0": wrap(z + k, nz)} for k in far_first(nz)]
    x_peers = [{"rows_1": wrap(x + k, nx), "tm_1": c} for k in far_first(nx) for c in (1 - core, core)]

    def greet(device):
        pl.semaphore_signal(barrier, inc=1, device_id=device, device_id_type=MESH)

    lead = core == 1
    for k in far_first(nz):
        pl.when(jnp.logical_and(lead, z + k < nz))(functools.partial(greet, {"rows_0": z + k}))
    for peer in y_peers + x_peers:
        greet(peer)
    crosses_up = jnp.logical_and(has_up, x == 0)
    crosses_down = jnp.logical_and(has_down, x == nx - 1)
    expected = len(y_peers) + len(x_peers) + jnp.where(lead, z, 0)
    if nx > 1:
        pl.when(crosses_up)(lambda: greet(up))
        pl.when(crosses_down)(lambda: greet(down))
        expected = expected + jnp.where(crosses_up, 1, 0) + jnp.where(crosses_down, 1, 0)

    for i, ref in enumerate((gamma, beta)):
        pltpu.make_async_copy(ref, consts.at[i], local_sem.at[1]).start()
    block = 3 * outs
    mine = pl.ds(pl.multiple_of(core * 3 * block, 16), 3 * block)
    for a in range(3):
        for b in range(3):
            pltpu.make_async_copy(
                kern.at[a, b],
                taps.at[pl.ds(pl.multiple_of(core * 3 * block + a * block, 16), block), pl.ds(b * channels, channels)],
                local_sem.at[2],
            ).start()

    lane = lax.broadcasted_iota(jnp.int32, (channels, LANES), 1)
    chan = lax.broadcasted_iota(jnp.int32, (channels, LANES), 0)
    member = jnp.where(chan // group == lane, 1.0, 0.0)

    def gather_groups(v):
        return lax.dot_general(v, member, (((1,), (0,)), ((), ())), precision=HIGHEST, preferred_element_type=jnp.float32)

    def spread_groups(v):
        return lax.dot_general(v, member, (((1,), (1,)), ((), ())), precision=HIGHEST, preferred_element_type=jnp.float32)

    acc[...] = jnp.zeros_like(acc)
    for unfolded in (wide_a, wide_b):
        unfolded[rows * width :, :] = jnp.zeros((width, 3 * channels), unfolded.dtype)

    own.wait()
    count = rows * width
    values = frames[pl.ds(home + 1, rows)].reshape(count, channels).astype(jnp.float32)
    mean_c = jnp.sum(values, axis=0, keepdims=True) * (1.0 / count)
    off = values - mean_c
    m2_c = jnp.sum(off * off, axis=0, keepdims=True)
    mean_c8 = jnp.broadcast_to(mean_c, (8, channels))
    mean_g = gather_groups(mean_c8) * (1.0 / group)
    apart = mean_c8 - spread_groups(mean_g)
    m2_g = gather_groups(m2_c + count * (apart * apart))
    stat_y[me] = jnp.concatenate([mean_g[0:1], m2_g[0:1]], axis=0)

    pl.semaphore_wait(barrier, expected)
    for k in far_first(nz):

        @pl.when(jnp.logical_and(lead, z - k >= 0))
        def _():
            pl.semaphore_signal(z_in, inc=1, device_id={"rows_0": z - k}, device_id_type=MESH)


    def publish(buf, at, peers, sem):
        for peer in peers:
            remote(buf.at[at], buf.at[at], sem.at[0], sem.at[1], peer).start()

    def several(buf, n, sem):
        return remote(buf.at[pl.ds(0, n)], buf.at[pl.ds(0, n)], sem.at[0], sem.at[1], partner)

    def collect(buf, peers, sem, weight):
        if peers:
            several(buf, len(peers), sem).wait_recv()
        means, m2s = buf[:, 0:1, :], buf[:, 1:2, :]
        mean = jnp.sum(means, axis=0) * (1.0 / buf.shape[0])
        gap = means - mean[None]
        m2 = jnp.sum(m2s, axis=0) + weight * jnp.sum(gap * gap, axis=0)
        return jnp.concatenate([mean, m2], axis=0)

    publish(stat_y, me, y_peers, y_sem)

    def ring_copy(src, way, chunk):
        at = frames.at[src * slot + 1 + chunk]
        return remote(at, at, ring_send, ring_recv.at[src, chunk], {"tm_0": y_next if way == 0 else y_prev})

    def halo_copy(src, side):
        at, to = (1, rows + 1) if side == 0 else (rows, 0)
        return remote(
            frames.at[src * slot + at], frames.at[src * slot + to], halo_send, halo_recv.at[src], up if side == 0 else down
        )

    def send_halo(src, chunk):
        if chunk == 0:
            pl.when(has_up)(lambda: halo_copy(src, 0).start())
        if chunk == last:
            pl.when(has_down)(lambda: halo_copy(src, 1).start())

    for chunk in ORDER:
        ring_copy(y, 0, chunk).start()
        ring_copy(y, 1, chunk).start()
    for chunk in (0, last):
        send_halo(y, chunk)

    pltpu.make_async_copy(taps.at[mine], taps.at[mine], local_sem.at[2]).wait()
    tap_remote = remote(taps.at[mine], taps.at[mine], tap_sem.at[0], tap_sem.at[1], partner)
    tap_remote.start()
    pltpu.make_async_copy(consts, consts, local_sem.at[1]).wait()

    def ring_event(step, chunk):
        for way in (0, 1):
            src = chip(-step) if way == 0 else chip(step)

            def arrive(src=src, way=way):
                ring_copy(src, way, chunk).wait_recv()
                if step < half - 1:
                    ring_copy(src, way, chunk).start()
                elif step == half - 1:
                    pl.when(core == way)(lambda: ring_copy(src, way, chunk).start())
                send_halo(src, chunk)

            if step < half:
                arrive()
            else:
                pl.when(core == way)(arrive)

    per_device = float(rows * width * group)
    early = [(step, chunk) for step in range(1, half - 1) for chunk in ORDER]

    def ring_events(todo):
        for step, chunk in todo:
            ring_event(step, chunk)

    ring_events(early[:1])
    span = collect(stat_y, y_peers, y_sem, per_device)

    @pl.when(lead)
    def _():
        stat_z[z] = span
        pl.when(z < nz - 1)(lambda: pl.semaphore_wait(z_in, nz - 1 - z))
        publish(stat_z, z, z_peers, z_sem)

    ring_events(early[1:])

    @pl.when(lead)
    def _():
        stat_x[x] = collect(stat_z, z_peers, z_sem, per_device * tms)
        publish(stat_x, x, x_peers + [partner], x_sem)

    late = [(step, chunk) for step in (half - 1, half) for chunk in ORDER]
    ring_events(late[: HEAD if ny >= 8 else 0])
    if nx > 1:
        pl.when(lead)(lambda: several(stat_x, nx - 1, x_sem).wait_recv())
    pl.when(jnp.logical_not(lead))(lambda: several(stat_x, nx, x_sem).wait_recv())
    final = collect(stat_x, (), x_sem, per_device * tms * nz)
    total = per_device * tms * nz * nx
    inv = lax.rsqrt(final[1:2] * (1.0 / total) + EPSILON)
    both = spread_groups(jnp.concatenate([final[0:1], inv] + [jnp.zeros((6, LANES), jnp.float32)], axis=0))
    affine[0:1] = both[0:1]
    affine[1:2] = 0.5 * both[1:2] * consts[0]
    affine[2:3] = 0.5 * consts[1]
    tap_remote.wait_recv()

    column = lax.rem(lax.broadcasted_iota(jnp.int32, (outs, wide), 1), width)
    at_left, at_right = column == 0, column == width - 1

    def source(k):
        if isinstance(k, int):
            return chip((k + 1) // 2 if k % 2 else -(k // 2))
        return chip(jnp.where(lax.rem(k, 2) == 1, (k + 1) // 2, -(k // 2)))

    def halo_wait(src):
        def rows_in(n):
            at = frames.at[pl.ds(0, n)]
            remote(at, at, halo_send, halo_recv.at[src], partner).wait_recv()

        pl.when(inner)(lambda: rows_in(2))
        pl.when(jnp.logical_not(inner))(lambda: rows_in(1))

    def prepare(src, unfolded):
        for r in range(rows + 2):
            value = frames[src * slot + r].astype(jnp.float32)
            h = (value - affine[0:1]) * affine[1:2] + affine[2:3]
            active = h + h * jnp.tanh(h)
            if r == 0:
                active = jnp.where(has_up, active, 0.0)
            if r == rows + 1:
                active = jnp.where(has_down, active, 0.0)
            active = active.astype(unfolded.dtype)
            for b in range(3):
                if 0 <= r - b < rows:
                    unfolded[(r - b) * width : (r - b + 1) * width, b * channels : (b + 1) * channels] = active

    def multiply(unfolded, product):
        for owner in (0, 1):
            part = slice(owner * 3 * block, (owner + 1) * 3 * block)
            product[part] = lax.dot_general(
                taps[part], unfolded[...], (((1,), (1,)), ((), ())), preferred_element_type=jnp.float32
            )

    def accumulate(src, product):
        frame = 2 * src + core
        totals = []
        for owner in (0, 1):
            for a in range(3):
                base = (owner * 3 + a) * block
                one, two, three = (product[base + c * outs : base + (c + 1) * outs] for c in range(3))
                one = jnp.where(at_left, 0.0, pltpu.roll(one, 1, 1))
                three = jnp.where(at_right, 0.0, pltpu.roll(three, wide - 1, 1))
                total = one + two + three
                acc[owner, frame + 2 - a] += total
                totals.append(total)
        return totals

    def repeat_first(src, totals):
        @pl.when(2 * src + core == 0)
        def _():
            for owner in (0, 1):
                acc[owner, 0] += totals[3 * owner] + totals[3 * owner + 1]
                acc[owner, 1] += totals[3 * owner]

    def released(j):
        if isinstance(j, int):
            return chip((j + 1) // 2 if j % 2 else 1 - j // 2)
        return chip(jnp.where(lax.rem(j, 2) == 1, (j + 1) // 2, 1 - j // 2))

    def part_copy(to):
        return remote(acc.at[1 - core, pl.ds(2 * to, 2)], arrived.at[to], part_send, part_recv.at[to], partner)

    low = lax.broadcasted_iota(jnp.int32, (outs // 2, LANES), 1) < width

    def finish(to):
        part_copy(to).wait_recv()
        for which in (0, 1):
            value = acc[core, 2 * to + which] + arrived[to, which]
            rest = value[:, LANES:]
            packed = jnp.where(low, rest[: outs // 2], pltpu.roll(rest[outs // 2 :], width, 1))
            value = jnp.concatenate([value[:, :LANES], packed], axis=0).astype(ready.dtype)
            stays = jnp.logical_and(to == y, core == which)

            @pl.when(stays)
            def _():
                result[me] = value

            @pl.when(jnp.logical_not(stays))
            def _():
                ready[2 * to + which] = value
                remote(ready.at[2 * to + which], result.at[me], back_sem.at[0], back_sem.at[1], {"tm_0": to, "tm_1": which}).start()

    if ny >= 8:
        events = {k: [late[e] for e in todo if e >= HEAD] for k, todo in PLAN.items()}
        events = {k: todo for k, todo in events.items() if todo}
    else:
        events = {1: late[:3], ny - 1: late[3:]}
    wides, prods = (wide_a, wide_b), (prod_a, prod_b)

    def arrivals(k):
        if isinstance(k, int):
            ring_events(events.get(k, []))
        else:
            for when, todo in events.items():
                pl.when(k == when)(functools.partial(ring_events, todo))
        halo_wait(source(k))

    def stage(i, parity):
        other = 1 - parity
        arrivals(i + 1)
        prepare(source(i + 1), wides[other])
        multiply(wides[parity], prods[parity])
        sums(i - 1, other)
        pl.when(i > 1)(lambda: part_copy(released(i - 1)).start())
        pl.when(i > 2)(lambda: finish(released(i - 2)))

    def sums(i, parity):
        repeat_first(source(i), accumulate(source(i), prods[parity]))

    arrivals(0)
    prepare(source(0), wide_a)
    arrivals(1)
    prepare(source(1), wide_b)
    multiply(wide_a, prod_a)

    @pl.loop(0, half - 2)
    def _(p):
        stage(2 * p + 1, 1)
        stage(2 * p + 2, 0)

    stage(ny - 3, 1)
    multiply(wide_a, prod_a)
    sums(ny - 3, 1)
    part_copy(released(ny - 3)).start()
    if ny > 4:
        finish(released(ny - 4))
    sums(ny - 2, 0)
    part_copy(released(ny - 2)).start()
    arrivals(ny - 1)
    prepare(source(ny - 1), wide_b)
    multiply(wide_b, prod_b)
    finish(released(ny - 3))
    sums(ny - 1, 1)
    part_copy(released(ny - 1)).start()
    part_copy(released(ny)).start()
    for j in range(ny - 2, ny + 1):
        finish(released(j))

    several(result, tms - 1, back_sem).wait_recv()
    conv = jnp.transpose(result[:, :outs].reshape(channels, LANES).astype(jnp.float32), (1, 0))
    out[0, : rows - 1] = conv.astype(out.dtype).reshape(rows - 1, width, channels)
    rest = result[:, outs:].astype(jnp.float32)
    rest = jnp.concatenate([rest, pltpu.roll(rest, width, 2)], axis=1).reshape(channels, LANES)
    rest = jnp.transpose(rest, (1, 0))[:width]
    out[0, last] = rest.astype(out.dtype)

    several(stat_y, tms - 1, y_sem).wait_send()
    several(ready, tms - 1, back_sem).wait_send()

    @pl.when(lead)
    def _():
        several(stat_z, nz - 1, z_sem).wait_send()
        several(stat_y, 2 * nx - 1, x_sem).wait_send()

    tap_remote.wait_send()

    def rows_out(n, sem):
        at = frames.at[pl.ds(0, n)]
        remote(at, at, sem, halo_recv.at[0], partner).wait_send()

    rows_out(rows * (2 * half - 1), ring_send)
    pl.when(inner)(lambda: rows_out(2 * ny, halo_send))
    pl.when(jnp.logical_not(inner))(lambda: rows_out(ny, halo_send))
    remote(arrived, arrived, part_send, part_recv.at[0], partner).wait_send()


def local(sizes, features, gamma, beta, kernel, bias):
    ny, nz, nx = sizes
    tms = 2 * ny
    _, rows, width, channels = features.shape
    outs = kernel.shape[1]
    taps = jnp.transpose(kernel, (0, 2, 3, 1, 4)).reshape(3, 3, 3 * outs, channels)
    wide = (rows + 1) * width
    bf16, f32 = jnp.bfloat16, jnp.float32
    dma = pltpu.SemaphoreType.DMA
    any_spec = pl.BlockSpec(memory_space=pltpu.HBM)
    vector = lambda v: v.reshape(1, channels)
    conv = pl.pallas_call(
        functools.partial(conv_kernel, sizes),
        out_shape=pltpu.VMEM(features.shape, bf16),
        in_specs=[any_spec] * 4,
        out_specs=pl.BlockSpec(memory_space=pltpu.VMEM),
        scratch_shapes=[
            pltpu.VMEM((ny * (rows + 2), width, channels), bf16),
            pltpu.VMEM((18 * outs, 3 * channels), bf16),
            pltpu.VMEM((wide, 3 * channels), bf16),
            pltpu.VMEM((wide, 3 * channels), bf16),
            pltpu.VMEM((18 * outs, wide), f32),
            pltpu.VMEM((18 * outs, wide), f32),
            pltpu.VMEM((2, tms + 2, outs, wide), f32),
            pltpu.VMEM((ny, 2, outs, wide), f32),
            pltpu.VMEM((tms, outs * 3 // 2, LANES), bf16),
            pltpu.VMEM((tms, outs * 3 // 2, LANES), bf16),
            pltpu.VMEM((2, 1, channels), f32),
            pltpu.VMEM((tms, 2, LANES), f32),
            pltpu.VMEM((nz, 2, LANES), f32),
            pltpu.VMEM((nx, 2, LANES), f32),
            pltpu.VMEM((8, channels), f32),
            dma((3,)), dma((2,)),
            dma, dma((ny, rows)),
            dma, dma((ny,)),
            pltpu.SemaphoreType.REGULAR,
            dma((2,)), dma((2,)), dma((2,)),
            dma, dma((ny,)),
            dma((2,)),
        ],
        compiler_params=pltpu.CompilerParams(collective_id=0, has_side_effects=True, vmem_limit_bytes=VMEM_LIMIT),
        name="fused_block",
    )(features, vector(gamma), vector(beta), taps)
    return (features.astype(f32) + conv.astype(f32) + bias).astype(bf16)


def solution(mesh):
    sizes = (8, 8, 4)
    split = Mesh(mesh.devices.reshape(8, 2, 8, 4), TM + ROWS)
    in_specs = (P(TM, ROWS, None, None), P(), P(), P(None, TM, None, None, None), P())
    out_specs = P(TM, ROWS, None, None)
    return jax.shard_map(
        functools.partial(local, sizes), mesh=split, in_specs=in_specs, out_specs=out_specs, check_vma=False
    )
```

```python
import functools

import jax
import jax.numpy as jnp
from jax import lax
from jax.experimental import pallas as pl
from jax.experimental.pallas import tpu as pltpu
from jax.sharding import Mesh
from jax.sharding import PartitionSpec as P

GROUPS = 32
EPSILON = 1e-06
TM = ("tm_0", "tm_1")
ROWS = ("rows_0", "rows_1")
HIGHEST = lax.Precision.HIGHEST
MESH = pl.DeviceIdType.MESH
LANES = 128
HEAD = 3
PLAN = {1: (3,), 2: (4,), 7: (5,)}
VMEM_LIMIT = 67043328 - 409600
ORDER = (0, 2, 1)


def conv_kernel(
    sizes, feat, gamma, beta, kern, out,
    frames, taps, wide_a, wide_b, prod_a, prod_b, acc, arrived, ready, result, consts, stat_y, stat_z, stat_x,
    affine, local_sem, tap_sem, ring_send, ring_recv, halo_send, halo_recv,
    z_in, y_sem, z_sem, x_sem, part_send, part_recv, back_sem,
):
    ny, nz, nx = sizes
    tms = 2 * ny
    half = ny // 2
    rows, width, channels = feat.shape[1:]
    outs = kern.shape[2] // 3
    group = channels // GROUPS
    wide = (rows + 1) * width
    last = rows - 1
    slot = rows + 2

    y, core = lax.axis_index("tm_0"), lax.axis_index("tm_1")
    z, x = lax.axis_index("rows_0"), lax.axis_index("rows_1")
    me = 2 * y + core
    row = z * nx + x
    has_up, has_down = row > 0, row < nz * nx - 1
    inner = jnp.logical_and(has_up, has_down)

    def wrap(v, n):
        v = jnp.where(v >= n, v - n, v)
        return jnp.where(v < 0, v + n, v)

    def chip(offset):
        return wrap(y + offset, ny)

    up = {"rows_0": jnp.where(x > 0, z, wrap(z - 1, nz)), "rows_1": jnp.where(x > 0, x - 1, nx - 1)}
    down = {"rows_0": jnp.where(x < nx - 1, z, wrap(z + 1, nz)), "rows_1": jnp.where(x < nx - 1, x + 1, 0)}
    y_next, y_prev = chip(1), chip(-1)
    partner = {"tm_1": 1 - core}
    home = y * slot

    def remote(src, dst, send, recv, device):
        return pltpu.make_async_remote_copy(
            src_ref=src, dst_ref=dst, send_sem=send, recv_sem=recv,
            device_id=device, device_id_type=MESH,
        )

    own = pltpu.make_async_copy(feat.at[0], frames.at[pl.ds(home + 1, rows)], local_sem.at[0])
    own.start()

    barrier = pltpu.get_barrier_semaphore()

    def far_first(n):
        return sorted(range(1, n), key=lambda k: -min(k, n - k))

    y_peers = [{"tm_0": chip(k), "tm_1": c} for k in far_first(ny) for c in (core, 1 - core)] + [partner]
    z_peers = [{"rows_0": wrap(z + k, nz)} for k in far_first(nz)]
    x_peers = [{"rows_1": wrap(x + k, nx), "tm_1": c} for k in far_first(nx) for c in (1 - core, core)]

    def greet(device):
        pl.semaphore_signal(barrier, inc=1, device_id=device, device_id_type=MESH)

    lead = core == 1
    for k in far_first(nz):
        pl.when(jnp.logical_and(lead, z + k < nz))(functools.partial(greet, {"rows_0": z + k}))
    for peer in y_peers + x_peers:
        greet(peer)
    crosses_up = jnp.logical_and(has_up, x == 0)
    crosses_down = jnp.logical_and(has_down, x == nx - 1)
    expected = len(y_peers) + len(x_peers) + jnp.where(lead, z, 0)
    if nx > 1:
        pl.when(crosses_up)(lambda: greet(up))
        pl.when(crosses_down)(lambda: greet(down))
        expected = expected + jnp.where(crosses_up, 1, 0) + jnp.where(crosses_down, 1, 0)

    for i, ref in enumerate((gamma, beta)):
        pltpu.make_async_copy(ref, consts.at[i], local_sem.at[1]).start()
    block = 3 * outs
    mine = pl.ds(pl.multiple_of(core * 3 * block, 16), 3 * block)
    for a in range(3):
        for b in range(3):
            pltpu.make_async_copy(
                kern.at[a, b],
                taps.at[pl.ds(pl.multiple_of(core * 3 * block + a * block, 16), block), pl.ds(b * channels, channels)],
                local_sem.at[2],
            ).start()

    lane = lax.broadcasted_iota(jnp.int32, (channels, LANES), 1)
    chan = lax.broadcasted_iota(jnp.int32, (channels, LANES), 0)
    member = jnp.where(chan // group == lane, 1.0, 0.0)

    def gather_groups(v):
        return lax.dot_general(v, member, (((1,), (0,)), ((), ())), precision=HIGHEST, preferred_element_type=jnp.float32)

    def spread_groups(v):
        return lax.dot_general(v, member, (((1,), (1,)), ((), ())), precision=HIGHEST, preferred_element_type=jnp.float32)

    acc[...] = jnp.zeros_like(acc)
    for unfolded in (wide_a, wide_b):
        unfolded[rows * width :, :] = jnp.zeros((width, 3 * channels), unfolded.dtype)

    own.wait()
    count = rows * width
    values = frames[pl.ds(home + 1, rows)].reshape(count, channels).astype(jnp.float32)
    mean_c = jnp.sum(values, axis=0, keepdims=True) * (1.0 / count)
    off = values - mean_c
    m2_c = jnp.sum(off * off, axis=0, keepdims=True)
    mean_c8 = jnp.broadcast_to(mean_c, (8, channels))
    mean_g = gather_groups(mean_c8) * (1.0 / group)
    apart = mean_c8 - spread_groups(mean_g)
    m2_g = gather_groups(m2_c + count * (apart * apart))
    stat_y[me] = jnp.concatenate([mean_g[0:1], m2_g[0:1]], axis=0)

    pl.semaphore_wait(barrier, expected)
    for k in far_first(nz):

        @pl.when(jnp.logical_and(lead, z - k >= 0))
        def _():
            pl.semaphore_signal(z_in, inc=1, device_id={"rows_0": z - k}, device_id_type=MESH)


    def publish(buf, at, peers, sem):
        for peer in peers:
            remote(buf.at[at], buf.at[at], sem.at[0], sem.at[1], peer).start()

    def several(buf, n, sem):
        return remote(buf.at[pl.ds(0, n)], buf.at[pl.ds(0, n)], sem.at[0], sem.at[1], partner)

    def collect(buf, peers, sem, weight):
        if peers:
            several(buf, len(peers), sem).wait_recv()
        means, m2s = buf[:, 0:1, :], buf[:, 1:2, :]
        mean = jnp.sum(means, axis=0) * (1.0 / buf.shape[0])
        gap = means - mean[None]
        m2 = jnp.sum(m2s, axis=0) + weight * jnp.sum(gap * gap, axis=0)
        return jnp.concatenate([mean, m2], axis=0)

    publish(stat_y, me, y_peers, y_sem)

    def ring_copy(src, way, chunk):
        at = frames.at[src * slot + 1 + chunk]
        return remote(at, at, ring_send, ring_recv.at[src, chunk], {"tm_0": y_next if way == 0 else y_prev})

    def halo_copy(src, side):
        at, to = (1, rows + 1) if side == 0 else (rows, 0)
        return remote(
            frames.at[src * slot + at], frames.at[src * slot + to], halo_send, halo_recv.at[src], up if side == 0 else down
        )

    def send_halo(src, chunk):
        if chunk == 0:
            pl.when(has_up)(lambda: halo_copy(src, 0).start())
        if chunk == last:
            pl.when(has_down)(lambda: halo_copy(src, 1).start())

    for chunk in ORDER:
        ring_copy(y, 0, chunk).start()
        ring_copy(y, 1, chunk).start()
    for chunk in (0, last):
        send_halo(y, chunk)

    pltpu.make_async_copy(taps.at[mine], taps.at[mine], local_sem.at[2]).wait()
    tap_remote = remote(taps.at[mine], taps.at[mine], tap_sem.at[0], tap_sem.at[1], partner)
    tap_remote.start()
    pltpu.make_async_copy(consts, consts, local_sem.at[1]).wait()

    def ring_event(step, chunk):
        for way in (0, 1):
            src = chip(-step) if way == 0 else chip(step)

            def arrive(src=src, way=way):
                ring_copy(src, way, chunk).wait_recv()
                if step < half - 1:
                    ring_copy(src, way, chunk).start()
                elif step == half - 1:
                    pl.when(core == way)(lambda: ring_copy(src, way, chunk).start())
                send_halo(src, chunk)

            if step < half:
                arrive()
            else:
                pl.when(core == way)(arrive)

    per_device = float(rows * width * group)
    early = [(step, chunk) for step in range(1, half - 1) for chunk in ORDER]

    def ring_events(todo):
        for step, chunk in todo:
            ring_event(step, chunk)

    ring_events(early[:1])
    span = collect(stat_y, y_peers, y_sem, per_device)

    @pl.when(lead)
    def _():
        stat_z[z] = span
        pl.when(z < nz - 1)(lambda: pl.semaphore_wait(z_in, nz - 1 - z))
        publish(stat_z, z, z_peers, z_sem)

    ring_events(early[1:])

    @pl.when(lead)
    def _():
        stat_x[x] = collect(stat_z, z_peers, z_sem, per_device * tms)
        publish(stat_x, x, x_peers + [partner], x_sem)

    late = [(step, chunk) for step in (half - 1, half) for chunk in ORDER]
    ring_events(late[: HEAD if ny >= 8 else 0])
    if nx > 1:
        pl.when(lead)(lambda: several(stat_x, nx - 1, x_sem).wait_recv())
    pl.when(jnp.logical_not(lead))(lambda: several(stat_x, nx, x_sem).wait_recv())
    final = collect(stat_x, (), x_sem, per_device * tms * nz)
    total = per_device * tms * nz * nx
    inv = lax.rsqrt(final[1:2] * (1.0 / total) + EPSILON)
    both = spread_groups(jnp.concatenate([final[0:1], inv] + [jnp.zeros((6, LANES), jnp.float32)], axis=0))
    affine[0:1] = both[0:1]
    affine[1:2] = 0.5 * both[1:2] * consts[0]
    affine[2:3] = 0.5 * consts[1]
    tap_remote.wait_recv()

    column = lax.rem(lax.broadcasted_iota(jnp.int32, (outs, wide), 1), width)
    at_left, at_right = column == 0, column == width - 1

    def source(k):
        if isinstance(k, int):
            return chip((k + 1) // 2 if k % 2 else -(k // 2))
        return chip(jnp.where(lax.rem(k, 2) == 1, (k + 1) // 2, -(k // 2)))

    def halo_wait(src):
        def rows_in(n):
            at = frames.at[pl.ds(0, n)]
            remote(at, at, halo_send, halo_recv.at[src], partner).wait_recv()

        pl.when(inner)(lambda: rows_in(2))
        pl.when(jnp.logical_not(inner))(lambda: rows_in(1))

    def prepare(src, unfolded):
        for r in range(rows + 2):
            value = frames[src * slot + r].astype(jnp.float32)
            h = (value - affine[0:1]) * affine[1:2] + affine[2:3]
            active = h + h * jnp.tanh(h)
            if r == 0:
                active = jnp.where(has_up, active, 0.0)
            if r == rows + 1:
                active = jnp.where(has_down, active, 0.0)
            active = active.astype(unfolded.dtype)
            for b in range(3):
                if 0 <= r - b < rows:
                    unfolded[(r - b) * width : (r - b + 1) * width, b * channels : (b + 1) * channels] = active

    def multiply(unfolded, product):
        for owner in (0, 1):
            part = slice(owner * 3 * block, (owner + 1) * 3 * block)
            product[part] = lax.dot_general(
                taps[part], unfolded[...], (((1,), (1,)), ((), ())), preferred_element_type=jnp.float32
            )

    def accumulate(src, product):
        frame = 2 * src + core
        totals = []
        for owner in (0, 1):
            for a in range(3):
                base = (owner * 3 + a) * block
                one, two, three = (product[base + c * outs : base + (c + 1) * outs] for c in range(3))
                one = jnp.where(at_left, 0.0, pltpu.roll(one, 1, 1))
                three = jnp.where(at_right, 0.0, pltpu.roll(three, wide - 1, 1))
                total = one + two + three
                acc[owner, frame + 2 - a] += total
                totals.append(total)
        return totals

    def repeat_first(src, totals):
        @pl.when(2 * src + core == 0)
        def _():
            for owner in (0, 1):
                acc[owner, 0] += totals[3 * owner] + totals[3 * owner + 1]
                acc[owner, 1] += totals[3 * owner]

    def released(j):
        if isinstance(j, int):
            return chip((j + 1) // 2 if j % 2 else 1 - j // 2)
        return chip(jnp.where(lax.rem(j, 2) == 1, (j + 1) // 2, 1 - j // 2))

    def part_copy(to):
        return remote(acc.at[1 - core, pl.ds(2 * to, 2)], arrived.at[to], part_send, part_recv.at[to], partner)

    low = lax.broadcasted_iota(jnp.int32, (outs // 2, LANES), 1) < width

    def finish(to):
        part_copy(to).wait_recv()
        for which in (0, 1):
            value = acc[core, 2 * to + which] + arrived[to, which]
            rest = value[:, LANES:]
            packed = jnp.where(low, rest[: outs // 2], pltpu.roll(rest[outs // 2 :], width, 1))
            value = jnp.concatenate([value[:, :LANES], packed], axis=0).astype(ready.dtype)
            stays = jnp.logical_and(to == y, core == which)

            @pl.when(stays)
            def _():
                result[me] = value

            @pl.when(jnp.logical_not(stays))
            def _():
                ready[2 * to + which] = value
                remote(ready.at[2 * to + which], result.at[me], back_sem.at[0], back_sem.at[1], {"tm_0": to, "tm_1": which}).start()

    if ny >= 8:
        events = {k: [late[e] for e in todo if e >= HEAD] for k, todo in PLAN.items()}
        events = {k: todo for k, todo in events.items() if todo}
    else:
        events = {1: late[:3], ny - 1: late[3:]}
    wides, prods = (wide_a, wide_b), (prod_a, prod_b)

    def arrivals(k):
        if isinstance(k, int):
            ring_events(events.get(k, []))
        else:
            for when, todo in events.items():
                pl.when(k == when)(functools.partial(ring_events, todo))
        halo_wait(source(k))

    def stage(i, parity):
        other = 1 - parity
        arrivals(i + 1)
        prepare(source(i + 1), wides[other])
        multiply(wides[parity], prods[parity])
        sums(i - 1, other)
        pl.when(i > 1)(lambda: part_copy(released(i - 1)).start())
        pl.when(i > 2)(lambda: finish(released(i - 2)))

    def sums(i, parity):
        repeat_first(source(i), accumulate(source(i), prods[parity]))

    arrivals(0)
    prepare(source(0), wide_a)
    arrivals(1)
    prepare(source(1), wide_b)
    multiply(wide_a, prod_a)

    @pl.loop(0, half - 2)
    def _(p):
        stage(2 * p + 1, 1)
        stage(2 * p + 2, 0)

    stage(ny - 3, 1)
    multiply(wide_a, prod_a)
    sums(ny - 3, 1)
    part_copy(released(ny - 3)).start()
    sums(ny - 2, 0)
    part_copy(released(ny - 2)).start()
    if ny > 4:
        finish(released(ny - 4))
    arrivals(ny - 1)
    prepare(source(ny - 1), wide_b)
    multiply(wide_b, prod_b)
    finish(released(ny - 3))
    sums(ny - 1, 1)
    part_copy(released(ny - 1)).start()
    part_copy(released(ny)).start()
    for j in range(ny - 2, ny + 1):
        finish(released(j))

    several(result, tms - 1, back_sem).wait_recv()
    conv = jnp.transpose(result[:, :outs].reshape(channels, LANES).astype(jnp.float32), (1, 0))
    out[0, : rows - 1] = conv.astype(out.dtype).reshape(rows - 1, width, channels)
    rest = result[:, outs:].astype(jnp.float32)
    rest = jnp.concatenate([rest, pltpu.roll(rest, width, 2)], axis=1).reshape(channels, LANES)
    rest = jnp.transpose(rest, (1, 0))[:width]
    out[0, last] = rest.astype(out.dtype)

    several(stat_y, tms - 1, y_sem).wait_send()
    several(ready, tms - 1, back_sem).wait_send()

    @pl.when(lead)
    def _():
        several(stat_z, nz - 1, z_sem).wait_send()
        several(stat_y, 2 * nx - 1, x_sem).wait_send()

    tap_remote.wait_send()

    def rows_out(n, sem):
        at = frames.at[pl.ds(0, n)]
        remote(at, at, sem, halo_recv.at[0], partner).wait_send()

    rows_out(rows * (2 * half - 1), ring_send)
    pl.when(inner)(lambda: rows_out(2 * ny, halo_send))
    pl.when(jnp.logical_not(inner))(lambda: rows_out(ny, halo_send))
    remote(arrived, arrived, part_send, part_recv.at[0], partner).wait_send()


def local(sizes, features, gamma, beta, kernel, bias):
    ny, nz, nx = sizes
    tms = 2 * ny
    _, rows, width, channels = features.shape
    outs = kernel.shape[1]
    taps = jnp.transpose(kernel, (0, 2, 3, 1, 4)).reshape(3, 3, 3 * outs, channels)
    wide = (rows + 1) * width
    bf16, f32 = jnp.bfloat16, jnp.float32
    dma = pltpu.SemaphoreType.DMA
    any_spec = pl.BlockSpec(memory_space=pltpu.HBM)
    vector = lambda v: v.reshape(1, channels)
    conv = pl.pallas_call(
        functools.partial(conv_kernel, sizes),
        out_shape=pltpu.VMEM(features.shape, bf16),
        in_specs=[any_spec] * 4,
        out_specs=pl.BlockSpec(memory_space=pltpu.VMEM),
        scratch_shapes=[
            pltpu.VMEM((ny * (rows + 2), width, channels), bf16),
            pltpu.VMEM((18 * outs, 3 * channels), bf16),
            pltpu.VMEM((wide, 3 * channels), bf16),
            pltpu.VMEM((wide, 3 * channels), bf16),
            pltpu.VMEM((18 * outs, wide), f32),
            pltpu.VMEM((18 * outs, wide), f32),
            pltpu.VMEM((2, tms + 2, outs, wide), f32),
            pltpu.VMEM((ny, 2, outs, wide), f32),
            pltpu.VMEM((tms, outs * 3 // 2, LANES), bf16),
            pltpu.VMEM((tms, outs * 3 // 2, LANES), bf16),
            pltpu.VMEM((2, 1, channels), f32),
            pltpu.VMEM((tms, 2, LANES), f32),
            pltpu.VMEM((nz, 2, LANES), f32),
            pltpu.VMEM((nx, 2, LANES), f32),
            pltpu.VMEM((8, channels), f32),
            dma((3,)), dma((2,)),
            dma, dma((ny, rows)),
            dma, dma((ny,)),
            pltpu.SemaphoreType.REGULAR,
            dma((2,)), dma((2,)), dma((2,)),
            dma, dma((ny,)),
            dma((2,)),
        ],
        compiler_params=pltpu.CompilerParams(collective_id=0, has_side_effects=True, vmem_limit_bytes=VMEM_LIMIT),
        name="fused_block",
    )(features, vector(gamma), vector(beta), taps)
    return (features.astype(f32) + conv.astype(f32) + bias).astype(bf16)


def solution(mesh):
    sizes = (8, 8, 4)
    split = Mesh(mesh.devices.reshape(8, 2, 8, 4), TM + ROWS)
    in_specs = (P(TM, ROWS, None, None), P(), P(), P(None, TM, None, None, None), P())
    out_specs = P(TM, ROWS, None, None)
    return jax.shard_map(
        functools.partial(local, sizes), mesh=split, in_specs=in_specs, out_specs=out_specs, check_vma=False
    )
```
